512 devices in a mesh: grp: 2 (over y), slab: 16 (over z), orb: 8 (over x), rep: 2 (over core).
Axes of the slice: x: 8, y: 2, z: 16, core: 2. Of those that a mesh axis runs over, the one named last changes fastest.
The devices are a block of a 8x8x16 slice.
Arguments:
- orbitals: bfloat16 [256, 32, 1024], P(('grp', 'slab', 'orb')), parts along dimension 0, may hold values from -6 to 6
- corners: int32 [256, 3], P('grp'), parts along dimension 0, may hold values from 0 to 191, as said below
- partners: int32 [256, 24], P(('grp', 'slab', 'orb')), parts along dimension 0, may hold values from -1 to 127, as said below
- kernel: float32 [32, 1024], replicated, may hold values from 0.05 to 5
Outputs:
- exchange_boxes: float32 [256, 32, 1024], P(('grp', 'slab', 'orb')), parts along dimension 0
- exchange_energy: float32 [2], P('grp'), parts along dimension 0
The draws below stay inside these ranges and needn't reach their ends.
There are 2 independent parts, one for each index of `grp`. The reference program is written for one: setup_inputs(seed, part) draws one part's arguments, and reference() takes and returns one part's arrays. A program takes and returns all parts, laid end to end along the dimension named above; an argument that names none is the same for every part. Nothing has to cross between parts.
Inputs may be any that keep to these rules, and one draw needn't show every extreme that they name: corners[i, 2] lies in the slab of orbital i: from 12 * (i // (1 * 8)) to 12 more less one; corners[i, 0] and corners[i, 1] lie below 192. `partners`: row i starts with i itself, names distinct orbitals whose boxes intersect box i (every component of o is above -32 and below 32), and has its -1 entries only after all others.
All inputs are finite; a program needn't handle non-finite values.
Results may differ from the reference program's by a relative error of at most 0.0003.
Values may be sent and summed in bfloat16 or wider, within the bound.
A program may use at most 64 MiB of HBM per device.

```python
import math
import jax
import jax.numpy as jnp
from jax import lax

B = 32
G = 192
ZDEV = 12
ORB_DEV = 1
NB = 24
NORB = 128
N_SLAB = 16
N_ORB = 8


def pair_tables(key):
    orbital_count = NORB
    group_size = ORB_DEV * N_ORB
    ranked_count = min(NB, NORB)
    subkeys = jax.random.split(key, 5)
    orbital_ids = jnp.arange(orbital_count, dtype=jnp.int32)
    slab_ids = orbital_ids // group_size
    corner_x = jnp.mod(jax.random.randint(subkeys[0], (orbital_count,), -B, B), G)
    corner_y = jnp.mod(jax.random.randint(subkeys[1], (orbital_count,), -B, B), G)
    corner_z = slab_ids * ZDEV + jax.random.randint(subkeys[2], (orbital_count,), 0, ZDEV)
    corners = jnp.stack([corner_x, corner_y, corner_z], axis=1).astype(jnp.int32)
    lengths = jnp.array([G, G, ZDEV * N_SLAB], jnp.int32)
    deltas = corners[:, None, :] - corners[None, :, :]
    halfway = lengths // 2
    offsets = jnp.mod(deltas + halfway, lengths) - halfway
    intersection = jnp.all(jnp.abs(offsets) < B, axis=2)
    random_rank = jax.random.randint(subkeys[3], (orbital_count, orbital_count), 0, (1 << 29) // orbital_count)
    scores = jnp.where(intersection, 1 << 30, 0) + random_rank * orbital_count + orbital_ids[None, :]
    scores = jnp.where(orbital_ids[:, None] == orbital_ids[None, :], jnp.int32(2147483647), scores).astype(jnp.int32)
    ranked = lax.top_k(scores, ranked_count)[1].astype(jnp.int32)
    picked = jnp.take_along_axis(intersection, ranked, axis=1)
    if ranked_count < NB:
        ranked = jnp.concatenate([ranked, jnp.zeros((orbital_count, NB - ranked_count), jnp.int32)], axis=1)
        picked = jnp.concatenate([picked, jnp.zeros((orbital_count, NB - ranked_count), bool)], axis=1)
    filled = jax.random.randint(subkeys[4], (orbital_count, 1), 1, NB + 1)
    slot_ids = jnp.arange(NB, dtype=jnp.int32)[None, :]
    usable = (slot_ids < filled) & picked
    partners = jnp.where(usable, ranked, -1).astype(jnp.int32)
    return (corners, partners)


def draw_corners(key, part):
    return pair_tables(jax.random.fold_in(key, 11))[0]


def draw_partners(key, part):
    return pair_tables(jax.random.fold_in(key, 11))[1]


def levels(own_key, shape, pieces, least, high):
    factor_of, own = 1.0, jax.random.fold_in(own_key, 6)
    for position, blocks in pieces:
        steps = jnp.exp(jax.random.uniform(jax.random.fold_in(own, position), (blocks,), jnp.float32, least / len(pieces), high / len(pieces)))
        factor_of = factor_of * jnp.repeat(steps, shape[position] // blocks).reshape([-1 if axis == position else 1 for axis in range(len(shape))])
    return factor_of


def normal_values(own_key, shape, width, reach, shards=(), held_as=jnp.bfloat16):
    gain = levels(own_key, shape, shards, -0.22, 0.18) if shards else 1.0
    result = jax.random.normal(own_key, shape, jnp.float32) * width * gain
    return jnp.minimum(jnp.maximum(result, -reach), reach).astype(held_as)


def setup_inputs(seed: int = 0, part: int = 0) -> dict:
    arg_keys = jax.random.split(jax.random.key(seed), 5)
    own_keys = jax.random.split(jax.random.fold_in(arg_keys[4], part), 5)
    return {
        "orbitals": normal_values(own_keys[0], (NORB, B, B * B), 1.0, 6.0, ((0, 128),)),
        "corners": draw_corners(jax.random.fold_in(jax.random.fold_in(arg_keys[4], part), 71), part),
        "partners": draw_partners(jax.random.fold_in(jax.random.fold_in(arg_keys[4], part), 71), part),
        "kernel": jnp.clip(jnp.exp(jax.random.uniform(arg_keys[3], (B, B * B), jnp.float32, math.log(0.05), math.log(5.0))), 0.05, 5.0),
    }


def wrapped(deltas, lengths):
    halfway = lengths // 2
    return jnp.mod(deltas + halfway, lengths) - halfway


def reference(orbitals, corners, partners, kernel):
    box_edge = orbitals.shape[1]
    box_count = orbitals.shape[0]
    cube_view = orbitals.reshape(box_count, box_edge, box_edge, box_edge)
    spectrum = kernel.reshape(box_edge, box_edge, box_edge)
    lengths = jnp.array([G, G, ZDEV * N_SLAB], jnp.int32)

    def one_orbital(orbital_id):
        centre = cube_view[orbital_id].astype(jnp.float32)
        corner = corners[orbital_id]

        def single_pair(partner):
            usable = partner >= 0
            safe_id = jnp.maximum(partner, 0).astype(jnp.int32)
            offset = wrapped(corner - corners[safe_id], lengths).astype(jnp.int32)
            padded = jnp.pad(cube_view[safe_id].astype(jnp.float32), box_edge)
            anchor = (offset + box_edge).astype(jnp.int32)
            shifted = lax.dynamic_slice(padded, (anchor[0], anchor[1], anchor[2]), (box_edge, box_edge, box_edge))
            shifted = jnp.where(usable, shifted, jnp.zeros_like(shifted))
            density = centre * shifted
            potential = jnp.real(jnp.fft.ifftn(spectrum * jnp.fft.fftn(density)))
            return potential * shifted, jnp.sum(density * potential)

        pair_terms, energies = lax.map(single_pair, partners[orbital_id])
        return -jnp.sum(pair_terms, axis=0), jnp.sum(energies)

    exchange_boxes, energies = lax.map(one_orbital, jnp.arange(box_count, dtype=jnp.int32))
    exchange_energy = -jnp.sum(energies) / (2.0 * box_count * box_edge ** 3)
    return exchange_boxes.reshape(box_count, box_edge, box_edge * box_edge), exchange_energy.reshape(1)
```

```python
import functools, math
import jax, jax.numpy as jnp, numpy as np
from jax import lax
from jax.experimental import pallas as pl
from jax.sharding import PartitionSpec as P
from jax.experimental.pallas import tpu as pltpu

G = 192
ZDEV = 12
B = 32
LANES = 128
PAIRS = 12
GROUPS = 3
MST = 392
F32 = jnp.float32
BF16 = jnp.bfloat16


def plane_tables():
    def th(q, p, bl, a):
        return 2 * np.pi * ((q * bl + p * a) % 32) / 32
    bl = np.repeat(np.arange(8), 32)[:, None]
    a = np.tile(np.arange(32), 8)[:, None]
    lane = np.arange(128)
    g, r = lane // 32, lane % 32
    q = np.where(g > 0, 4 * g, np.where(r < 16, 0, 16))
    p = np.where(g > 0, r, r % 16)
    t = th(q, p, bl, a)
    w0 = np.concatenate([np.cos(t), -np.sin(t)], 1)
    for l in (0, 16):
        w0[:, 128 + l] = np.cos(th(q[l], 16, bl, a))[:, 0]
    t = th(2 + 4 * g, r, bl, a)
    w2 = np.concatenate([np.cos(t), -np.sin(t)], 1)
    l2 = np.arange(256)
    t = th(1 + 4 * (l2 // 32), l2 % 32, bl, a)
    c, s = np.cos(t), np.sin(t)
    w1 = np.block([[c, -s], [s, c]])
    out = []
    for w in (w0, w2, w1):
        w = w.astype(np.float32)
        hi = w.astype(jnp.bfloat16)
        lo = (w - hi.astype(np.float32)).astype(jnp.bfloat16)
        out += [hi, lo]
    return out


def split(x):
    hi = x.astype(BF16)
    return hi, (x - hi.astype(F32)).astype(BF16)


def swap_tile(x):
    t = x.T
    return jnp.concatenate([t[32 * j:32 * j + 32] for j in range(4)], axis=1)


def fft16(re, im, sign):
    def four(a, b, c, d):
        (ar, ai), (br, bi), (cr, ci), (dr, di) = a, b, c, d
        sr, si, tr, ti = ar + cr, ai + ci, ar - cr, ai - ci
        ur, ui, vr, vi = br + dr, bi + di, br - dr, bi - di
        if sign < 0:
            wr, wi = vi, -vr
            return (sr + ur, si + ui), (tr + vi, ti - vr), (sr - ur, si - ui), (tr - vi, ti + vr)
        return (sr + ur, si + ui), (tr - vi, ti + vr), (sr - ur, si - ui), (tr + vi, ti - vr)

    x = list(zip(re, im))
    mid = [four(x[n], x[n + 4], x[n + 8], x[n + 12]) for n in range(4)]
    out = [None] * 16
    h = np.float32(math.sqrt(0.5))
    for k1 in range(4):
        col = []
        for n2 in range(4):
            zr, zi = mid[n2][k1]
            m = n2 * k1
            if m == 0:
                pass
            elif m == 4:
                zr, zi = (zi, -zr) if sign < 0 else (-zi, zr)
            elif m == 2:
                zr, zi = ((zr + zi) * h, (zi - zr) * h) if sign < 0 else ((zr - zi) * h, (zi + zr) * h)
            elif m == 6:
                zr, zi = ((zi - zr) * h, -(zr + zi) * h) if sign < 0 else (-(zr + zi) * h, (zr - zi) * h)
            else:
                c = np.float32(math.cos(2 * math.pi * m / 16))
                s = np.float32(sign * math.sin(2 * math.pi * m / 16))
                zr, zi = zr * c - zi * s, zr * s + zi * c
            col.append((zr, zi))
        res = four(*col)
        for k2 in range(4):
            out[k1 + 4 * k2] = res[k2]
    return [o[0] for o in out], [o[1] for o in out]


def own_tiles(x_ref):
    return [swap_tile(x_ref[0, :, LANES * t:LANES * t + LANES].astype(F32)) for t in range(8)]


def place_centre(tiles, cen):
    for t in range(8):
        for pair in range(4):
            cen[pl.ds(t * 128 + pair, 32, stride=4), :] = tiles[t]


def spectral_kernel(kern_ref, ksp, kdp):
    tiles = [swap_tile(kern_ref[:, LANES * t:LANES * t + LANES]) for t in range(8)]
    whole = jnp.concatenate(tiles, axis=0)

    def exact(a, f):
        one = a.astype(BF16)
        rest = a - one.astype(F32)
        two = rest.astype(BF16)
        three = (rest - two.astype(F32)).astype(BF16)
        return f(one) + (f(two) + f(three))
    row = lax.broadcasted_iota(jnp.int32, (LANES, LANES), 0)
    col = lax.broadcasted_iota(jnp.int32, (LANES, LANES), 1)
    mirror = jnp.bitwise_and(-jnp.bitwise_and(col, 96), 96) + jnp.bitwise_and(-col, 31)
    perm = jnp.where(row == mirror, 1.0, 0.0).astype(BF16)
    row = lax.broadcasted_iota(jnp.int32, (32, 32), 0)
    col = lax.broadcasted_iota(jnp.int32, (32, 32), 1)
    flip = jnp.where(row == jnp.bitwise_and(-col, 31), 1.0, 0.0).astype(BF16)
    lanes = exact(whole, lambda v: jnp.dot(v, perm, preferred_element_type=F32))
    rev = [lanes[32 * t:32 * t + 32] for t in range(8)]
    wide = jnp.concatenate(rev, axis=1)
    wide = exact(wide, lambda v: jnp.dot(flip, v, preferred_element_type=F32))
    rev = [wide[:, LANES * t:LANES * t + LANES] for t in range(8)]
    lane = lax.broadcasted_iota(jnp.int32, (32, LANES), 1)
    sym = []
    for t in range(8):
        other = jnp.where(lane < 32, rev[(8 - t) % 8], rev[7 - t])
        sym.append((tiles[t] + other) * np.float32(0.5))

    def groups(parts):
        out = None
        for g, (t, j) in enumerate(parts):
            v = sym[t]
            if (g - j) % 4:
                v = pltpu.roll(v, 32 * ((g - j) % 4), 1)
            out = v if out is None else jnp.where(lane >= 32 * g, v, out)
        return out
    scale = np.float32(2.0 / 32768)
    u0 = groups([(0, 0), (1, 0), (2, 0), (3, 0)])
    edge = pltpu.roll(sym[4], 16, 1)
    u0 = jnp.where((lane >= 16) & (lane < 32), edge, u0)
    u0 = u0 * scale
    half = np.float32(1.0 / 65536)
    first = sym[0]
    second = pltpu.roll(sym[0], LANES - 16, 1)
    third = sym[4]
    mean0, diff0 = (first + second) * half, (first - second) * half
    fourth = pltpu.roll(sym[4], LANES - 16, 1)
    mean1, diff1 = (third + fourth) * half, (third - fourth) * half
    mean1, diff1 = pltpu.roll(mean1, 16, 1), pltpu.roll(diff1, 16, 1)
    u0 = jnp.where(lane == 0, mean0, jnp.where(lane == 16, mean1, u0))
    d0 = jnp.where(lane == 0, diff0, jnp.where(lane == 16, diff1, jnp.zeros_like(diff0)))
    u1 = groups([(t, 2) for t in range(4)]) * scale
    u2 = groups([(t, 1) for t in range(4)]) * scale
    u3 = groups([(t + 4, 1) for t in range(4)]) * scale
    for pair in range(4):
        for u, v in enumerate((u0, u1, u2, u3)):
            ksp[pl.ds(u * 128 + pair, 16, stride=8), :] = v[:16]
            ksp[pl.ds(u * 128 + 4 + pair, 16, stride=8), :] = v[16:]
        kdp[pl.ds(pair, 16, stride=8), :] = d0[:16]
        kdp[pl.ds(4 + pair, 16, stride=8), :] = d0[16:]


def shift_boxes(pool, tab, zero_block, blocks, m):
    lane = lax.broadcasted_iota(jnp.int32, (8, LANES), 1)
    sub = lax.broadcasted_iota(jnp.int32, (8, LANES), 0)
    a_id = jnp.bitwise_and(lane, 31)
    b_id = sub * 4 + lax.shift_right_logical(lane, 5)

    def one(k, _):
        block, oc, ob, oa, use = tab(k)
        s = ob * 32 + oa
        r = jnp.bitwise_and(s, 127)
        sh = jnp.bitwise_and(lax.shift_right_arithmetic(s, 7), 7)
        lane_by = jnp.bitwise_and(128 - r, 127)
        sub_by = jnp.bitwise_and(8 - sh, 7)
        keep = (a_id + oa >= 0) & (a_id + oa < 32) & (b_id + ob >= 0) & (b_id + ob < 32)
        near = lane < 128 - r
        row = (k // 4) * 128 + k % 4
        for c in range(32):
            src = c + oc
            good = (src >= 0) & (src < 32) & use
            at = jnp.where(good, block + jnp.bitwise_and(src, 1) * blocks, zero_block)
            plane = jnp.where(good, lax.shift_right_arithmetic(src, 1), 0)
            v = pool[at, plane].astype(F32)
            v = pltpu.roll(v, lane_by, 1)
            v = pltpu.roll(v, sub_by, 0)
            w = pltpu.roll(v, 7, 0)
            v = jnp.where(keep, jnp.where(near, v, w), 0.0)
            m[pl.ds(row + 4 * c, 8, stride=MST), :] = v
        return 0
    lax.fori_loop(0, PAIRS, one, 0)


def densities(m, cen, yh, yl):
    def one(i, _):
        row = pl.multiple_of(i * 16, 16)
        crow = pl.multiple_of(jnp.bitwise_and(i, 7) * 16, 16)
        x = [m[pl.ds(pl.multiple_of(MST * t + row, 8), 16), :]
             * cen[pl.ds(pl.multiple_of(128 * t + crow, 16), 16), :] for t in range(8)]
        for h in range(2):
            e, o = x[h] + x[4 + h], x[2 + h] + x[6 + h]
            d, g = x[h] - x[4 + h], x[6 + h] - x[2 + h]
            for at, v in ((0, e + o), (256, e - o), (512, d), (768, g)):
                hi, lo = split(v)
                yh[pl.ds(row, 16), at + LANES * h:at + LANES * h + LANES] = hi
                yl[pl.ds(row, 16), at + LANES * h:at + LANES * h + LANES] = lo
        return 0
    lax.fori_loop(0, 24, one, 0)


CUTS = ((0, 256), (256, 512), (512, 1024))


def turn(yh, yl, w, s, back):
    for (b, e), (wh, wl) in zip(CUTS, w):
        hi, lo = yh[:, b:e], yl[:, b:e]
        dims = (((1,), (1 if back else 0,)), ((), ()))

        def dot(p, q):
            return lax.dot_general(p, q, dims, preferred_element_type=F32)
        out = dot(hi, wh[...]) + dot(lo, wh[...]) + dot(hi, wl[...])
        for t in range(b // LANES, e // LANES):
            s[t] = out[:, t * LANES - b:t * LANES - b + LANES]


def filtered(s, yh, yl, ksp, kdp):
    sub = lax.broadcasted_iota(jnp.int32, (8, LANES), 0)
    lower = sub < 4
    sgn = jnp.where(lower, np.float32(1), np.float32(-1))

    def twiddle(k):
        c = np.float32(math.cos(2 * math.pi * k / 32))
        n = np.float32(math.sin(2 * math.pi * k / 32))
        return jnp.where(lower, np.float32(1), c), jnp.where(lower, np.float32(0), n)

    def job(g, tr, ti, krow, special, energy):
        row = pl.multiple_of(g * 128, 128)
        re = [s[tr, pl.ds(row + 8 * n, 8), :] for n in range(16)]
        im = [s[ti, pl.ds(row + 8 * n, 8), :] for n in range(16)]
        re, im = fft16(re, im, -1)
        zr, zi = [], []
        for k in range(16):
            r, i = re[k], im[k]
            if k:
                c, n = twiddle(k)
                r, i = r * c + i * n, i * c - r * n
            zr.append(pltpu.roll(r, 4, 0) + sgn * r)
            zi.append(pltpu.roll(i, 4, 0) + sgn * i)
        wr, wi = [], []
        for k in range(16):
            km = ksp[pl.ds(krow + 8 * k, 8), :]
            r, i = zr[k] * km, zi[k] * km
            if special:
                kd = kdp[pl.ds(8 * k, 8), :]
                fr, fi = zr[(16 - k) % 16], zi[(16 - k) % 16]
                if k:
                    fr, fi = pltpu.roll(fr, 4, 0), pltpu.roll(fi, 4, 0)
                r, i = r + kd * fr, i - kd * fi
            energy = energy + (r * zr[k] + i * zi[k])
            wr.append(r)
            wi.append(i)
        re, im = [], []
        for k in range(16):
            r = pltpu.roll(wr[k], 4, 0) + sgn * wr[k]
            i = pltpu.roll(wi[k], 4, 0) + sgn * wi[k]
            if k:
                c, n = twiddle(k)
                r, i = r * c - i * n, i * c + r * n
            re.append(r)
            im.append(i)
        re, im = fft16(re, im, 1)
        for n in range(0, 16, 2):
            for t, z in ((tr, re), (ti, im)):
                hi, lo = split(jnp.concatenate([z[n], z[n + 1]], axis=0))
                at = pl.ds(row + 8 * n, 16)
                lanes = pl.ds(pl.multiple_of(t * LANES, LANES), LANES)
                yh[at, lanes] = hi
                yl[at, lanes] = lo
        return energy

    energy = jnp.zeros((8, LANES), F32)

    def first(g, e):
        return job(g, 0, 1, 0, True, e)

    def other(i, e):
        g, u = i // 3, i % 3 + 1
        tr = jnp.where(u == 1, 2, u + 2)
        ti = jnp.where(u == 1, 3, u + 4)
        return job(g, tr, ti, pl.multiple_of(u * 128, 128), False, e)
    energy = lax.fori_loop(0, GROUPS, first, energy)
    return lax.fori_loop(0, 3 * GROUPS, other, energy)


def collect(s, m, acc):
    def one(i, _):
        row = pl.multiple_of(i * 8, 8)
        for h in range(2):
            total = [None] * 4
            for g in range(GROUPS):
                y0, y2, yr, yi = (s[2 * n + h, pl.ds(g * 128 + row, 8), :] for n in range(4))
                p, q = y0 + y2, y0 - y2
                for n, v in enumerate((p + yr, q - yi, p - yr, q + yi)):
                    v = v * m[pl.ds(MST * (2 * n + h) + g * 128 + row, 8), :]
                    total[n] = v if total[n] is None else total[n] + v
            for n in range(4):
                acc[pl.ds((2 * n + h) * 128 + row, 8), :] = total[n]
        return 0
    lax.fori_loop(0, 16, one, 0)


def summed_tiles(acc):
    out = []
    for t in range(8):
        v = [acc[pl.ds(t * 128 + pair, 32, stride=4), :] for pair in range(4)]
        out.append((v[0] + v[1]) + (v[2] + v[3]))
    return out


HALO = 3
KEEP = {0: (0, 16), 1: (0, 16), 2: (0, 10), 3: (0, 4), -1: (0, 16), -2: (6, 10), -3: (12, 4)}
MESH = pl.DeviceIdType.MESH


def sign(v):
    return (v > 0) - (v < 0)


def routes(n_orb):
    out = []
    for core in range(2):
        tree = {}
        for dz in range(-HALO, HALO + 1):
            for dx in range(1 - n_orb // 2, n_orb // 2 + 1):
                if (dz, dx) == (0, 0):
                    continue
                way = sign(dx)
                if dx == n_orb // 2 and core == 1 and dz in (0, -1, -2):
                    way = -1
                if core == 0:
                    tree[dz, dx] = (sign(dz), 0) if dz else (0, way)
                else:
                    tree[dz, dx] = (0, way) if dx else (sign(dz), 0)
        out.append(tree)
    return out


def schedule(tree, core):
    def steps(p):
        dz, dx = p
        return (abs(dz) + abs(dx), abs(dx) if core == 0 else abs(dz), p)
    return sorted(tree, key=steps)


def kernel_body(n_slab, n_orb, x_ref, corners, partners, kern_hbm, *rest):
    w_hbm, rest = rest[:6], rest[6:]
    out_ref, en_ref = rest[:2]
    (pool, m, yh, yl, s, ksp, kdp, cen, acc, kern, part, other, echip, ex, ez) = rest[2:17]
    w_ref = rest[17:23]
    local_sem, send_sem, recv_sem, swap_send, swap_recv, tail_sem, ready_one, ready_two = rest[23:]
    here_x = lax.axis_index("orb")
    here_z = lax.axis_index("slab")
    rep = lax.axis_index("rep")
    blocks = (2 * HALO + 1) * n_orb
    zero_block = 2 * blocks

    loads = [pltpu.make_async_copy(kern_hbm, kern, local_sem.at[0])]
    loads += [pltpu.make_async_copy(a, b, local_sem.at[1 + i]) for i, (a, b) in enumerate(zip(w_hbm, w_ref))]
    for load in loads:
        load.start()

    def at_slab(step):
        return {"slab": lax.rem(here_z + step + n_slab, n_slab)}

    def at_orb(step):
        return {"orb": lax.rem(here_x + step + n_orb, n_orb)}
    sibling = {"rep": 1 - rep}

    barrier = pltpu.get_barrier_semaphore()
    for peer in (at_orb(1), at_orb(-1), at_slab(1), at_slab(-1), sibling):
        pl.semaphore_signal(barrier, inc=1, device_id=peer, device_id_type=MESH)

    tiles = own_tiles(x_ref)
    for t in range(8):
        acc[pl.ds(t, 32, stride=8), :] = tiles[t]
    own_block = HALO * n_orb + here_x
    mine = rep * blocks + own_block
    for c in range(16):
        even = acc[16 * c:16 * c + 8, :]
        odd = acc[16 * c + 8:16 * c + 16, :]
        pool[mine, c] = jnp.where(rep == 0, even, odd).astype(BF16)
    pool[zero_block, 0] = jnp.zeros((8, LANES), BF16)
    pl.semaphore_wait(barrier, 5)

    def slot(core, p):
        first, count = KEEP[p[0]]
        block = core * blocks + (p[0] + HALO) * n_orb + lax.rem(here_x + p[1] + n_orb, n_orb)
        return pool.at[block, pl.ds(first, count)]

    def index(p):
        return (p[0] + HALO) * n_orb + (p[1] + n_orb) % n_orb

    def swap(core, p):
        return pltpu.make_async_remote_copy(
            src_ref=slot(core, p), dst_ref=slot(core, p), send_sem=swap_send.at[index(p)],
            recv_sem=swap_recv.at[index(p)], device_id=sibling, device_id_type=MESH)

    def pass_on(core, p, hop):
        first, count = KEEP[p[0]]
        held = (p[0] - hop[0], p[1] - hop[1])
        x_slot = lax.rem(here_x + held[1] + n_orb, n_orb)
        src = pool.at[core * blocks + (held[0] + HALO) * n_orb + x_slot, pl.ds(first, count)]
        dst = pool.at[core * blocks + (p[0] + HALO) * n_orb + x_slot, pl.ds(first, count)]
        peer = at_slab(-hop[0]) if hop[0] else at_orb(-hop[1])
        return pltpu.make_async_remote_copy(
            src_ref=src, dst_ref=dst, send_sem=send_sem.at[index(p)], recv_sem=recv_sem.at[index(p)],
            device_id=peer, device_id_type=MESH)

    def arrival(core, p):
        return pltpu.make_async_remote_copy(
            src_ref=slot(core, p), dst_ref=slot(core, p), send_sem=send_sem.at[index(p)],
            recv_sem=recv_sem.at[index(p)], device_id=sibling, device_id_type=MESH)

    trees = routes(n_orb)

    def spread(core, held):
        for p, hop in trees[core].items():
            h = (p[0] - hop[0], p[1] - hop[1])
            if h == held or (h[0] == held[0] and (h[1] - held[1]) % n_orb == 0):
                pass_on(core, p, hop).start()
        swap(core, held).start()

    for core in range(2):
        @pl.when(rep == core)
        def _(core=core):
            spread(core, (0, 0))

    place_centre(tiles, cen)
    loads[0].wait()
    spectral_kernel(kern, ksp, kdp)

    for core in range(2):
        @pl.when(rep == core)
        def _(core=core):
            for p in schedule(trees[core], core):
                arrival(core, p).wait_recv()
                spread(core, p)
            for p in trees[core]:
                arrival(core, p).wait_send()
            for p in [(0, 0)] + list(trees[core]):
                swap(core, p).wait_send()
                swap(1 - core, p).wait_recv()

    def signal_far(sem):
        for step in (HALO, -HALO):
            pl.semaphore_signal(sem, inc=1, device_id=at_slab(step), device_id_type=MESH)
    signal_far(ready_one)

    own = here_z * n_orb + here_x

    def wrap(v):
        v = v + G // 2
        v = jnp.where(v < 0, v + G, jnp.where(v >= G, v - G, v))
        return v - G // 2

    def tab(k):
        j = partners[0, 2 * k + rep]
        use = j >= 0
        j = jnp.where(use, j, own)
        o = [wrap(corners[own, d] - corners[j, d]) for d in range(3)]
        dz = lax.div(j, n_orb) - here_z
        dz = jnp.where(dz > n_slab // 2, dz - n_slab, jnp.where(dz < -(n_slab // 2), dz + n_slab, dz))
        dz = jnp.clip(dz, -HALO, HALO)
        return (dz + HALO) * n_orb + lax.rem(j, n_orb), o[2], o[1], o[0], use

    shift_boxes(pool, tab, zero_block, blocks, m)
    densities(m, cen, yh, yl)
    for load in loads[1:]:
        load.wait()
    w = ((w_ref[0], w_ref[1]), (w_ref[2], w_ref[3]), (w_ref[4], w_ref[5]))
    pl.semaphore_wait(ready_one, 2)
    signal_far(ready_two)
    turn(yh, yl, w, s, False)
    energy = filtered(s, yh, yl, ksp, kdp)
    pl.semaphore_wait(ready_two, 2)

    echip[0] = jnp.sum(energy, axis=0, keepdims=True)
    swap_energy = pltpu.make_async_remote_copy(
        src_ref=echip.at[0], dst_ref=echip.at[1], send_sem=tail_sem.at[0], recv_sem=tail_sem.at[1],
        device_id=sibling, device_id_type=MESH)
    swap_energy.start()
    turn(yh, yl, w, s, True)
    swap_energy.wait()
    ex[here_x] = echip[0] + echip[1]

    def to_all(buf, here, size, at, sems):
        copies = []
        for step in range(1, size):
            copies.append(pltpu.make_async_remote_copy(
                src_ref=buf.at[here], dst_ref=buf.at[here], send_sem=sems[0].at[sems[1] + step],
                recv_sem=sems[0].at[sems[1] + size + step], device_id=at(step), device_id_type=MESH))
        return copies

    def from_all(buf, here, size, at, sems):
        for step in range(1, size):
            there = lax.rem(here - step + size, size)
            pltpu.make_async_remote_copy(
                src_ref=buf.at[there], dst_ref=buf.at[there], send_sem=sems[0].at[sems[1] + step],
                recv_sem=sems[0].at[sems[1] + size + step], device_id=at(step), device_id_type=MESH).wait_recv()
    x_sems = (tail_sem, 4)
    z_sems = (tail_sem, 4 + 2 * n_orb)
    x_copies = to_all(ex, here_x, n_orb, at_orb, x_sems)
    for copy in x_copies:
        copy.start()
    collect(s, m, acc)
    res = summed_tiles(acc)
    for t in range(8):
        part[t] = res[t]
    swap_part = pltpu.make_async_remote_copy(
        src_ref=part, dst_ref=other, send_sem=tail_sem.at[2], recv_sem=tail_sem.at[3],
        device_id=sibling, device_id_type=MESH)
    swap_part.start()
    from_all(ex, here_x, n_orb, at_orb, x_sems)
    ez[here_z] = functools.reduce(lambda a, b: a + b, [ex[i] for i in range(n_orb)])
    z_copies = to_all(ez, here_z, n_slab, at_slab, z_sems)
    for copy in z_copies:
        copy.start()
    swap_part.wait()
    for t in range(8):
        out_ref[0, :, LANES * t:LANES * t + LANES] = -swap_tile(part[t] + other[t])
    for copy in x_copies:
        copy.wait_send()
    from_all(ez, here_z, n_slab, at_slab, z_sems)
    total = functools.reduce(lambda a, b: a + b, [ez[i] for i in range(n_slab)])
    for copy in z_copies:
        copy.wait_send()
    en_ref[0] = jnp.sum(total) * np.float32(-1.0 / (2.0 * n_slab * n_orb * B ** 3))


def body(n_slab, n_orb, orbitals, corners, partners, kernel):
    blocks = (2 * HALO + 1) * n_orb
    vmem = pl.BlockSpec(memory_space=pltpu.VMEM)
    smem = pl.BlockSpec(memory_space=pltpu.SMEM)
    hbm = pl.BlockSpec(memory_space=pl.ANY)
    dma = pltpu.SemaphoreType.DMA
    weights = [jnp.asarray(w) for w in plane_tables()]
    return pl.pallas_call(
        functools.partial(kernel_body, n_slab, n_orb),
        out_shape=(jax.ShapeDtypeStruct((1, B, B * B), F32), jax.ShapeDtypeStruct((1,), F32)),
        in_specs=[vmem, smem, smem, hbm] + [hbm] * 6,
        out_specs=(vmem, smem),
        scratch_shapes=[
            pltpu.VMEM((2 * blocks + 1, 16, 8, LANES), BF16),
            pltpu.VMEM((8 * MST, LANES), F32),
            pltpu.VMEM((384, 1024), BF16),
            pltpu.VMEM((384, 1024), BF16),
            pltpu.VMEM((8, 384, LANES), F32),
            pltpu.VMEM((512, LANES), F32),
            pltpu.VMEM((128, LANES), F32),
            pltpu.VMEM((1024, LANES), F32),
            pltpu.VMEM((1024, LANES), F32),
            pltpu.VMEM((B, B * B), F32),
            pltpu.VMEM((8, B, LANES), F32),
            pltpu.VMEM((8, B, LANES), F32),
            pltpu.VMEM((2, 1, LANES), F32),
            pltpu.VMEM((n_orb, 1, LANES), F32),
            pltpu.VMEM((n_slab, 1, LANES), F32),
            *[pltpu.VMEM(w.shape, BF16) for w in weights],
            dma((7,)),
            dma((blocks,)),
            dma((blocks,)),
            dma((blocks,)),
            dma((blocks,)),
            dma((4 + 2 * n_orb + 2 * n_slab,)),
            pltpu.SemaphoreType.REGULAR,
            pltpu.SemaphoreType.REGULAR,
        ],
        compiler_params=pltpu.CompilerParams(
            collective_id=0, has_side_effects=True, vmem_limit_bytes=48 * 2**20),
    )(orbitals, corners, partners, kernel, *weights)


def solution(mesh):
    in_specs = (
        P(("grp", "slab", "orb"), None, None),
        P("grp", None),
        P(("grp", "slab", "orb"), None),
        P(),
    )
    out_specs = (P(("grp", "slab", "orb"), None, None), P("grp"))
    step = functools.partial(body, mesh.shape["slab"], mesh.shape["orb"])
    return jax.shard_map(step, mesh=mesh, in_specs=in_specs, out_specs=out_specs, check_vma=False)
```

```python
import functools, math
import jax, jax.numpy as jnp, numpy as np
from jax import lax
from jax.experimental import pallas as pl
from jax.sharding import PartitionSpec as P
from jax.experimental.pallas import tpu as pltpu

G = 192
ZDEV = 12
B = 32
LANES = 128
PAIRS = 12
GROUPS = 3
MST = 392
F32 = jnp.float32
BF16 = jnp.bfloat16


def plane_tables():
    def th(q, p, bl, a):
        return 2 * np.pi * ((q * bl + p * a) % 32) / 32
    bl = np.repeat(np.arange(8), 32)[:, None]
    a = np.tile(np.arange(32), 8)[:, None]
    lane = np.arange(128)
    g, r = lane // 32, lane % 32
    q = np.where(g > 0, 4 * g, np.where(r < 16, 0, 16))
    p = np.where(g > 0, r, r % 16)
    t = th(q, p, bl, a)
    w0 = np.concatenate([np.cos(t), -np.sin(t)], 1)
    for l in (0, 16):
        w0[:, 128 + l] = np.cos(th(q[l], 16, bl, a))[:, 0]
    t = th(2 + 4 * g, r, bl, a)
    w2 = np.concatenate([np.cos(t), -np.sin(t)], 1)
    l2 = np.arange(256)
    t = th(1 + 4 * (l2 // 32), l2 % 32, bl, a)
    c, s = np.cos(t), np.sin(t)
    w1 = np.block([[c, -s], [s, c]])
    out = []
    for w in (w0, w2, w1):
        w = w.astype(np.float32)
        hi = w.astype(jnp.bfloat16)
        lo = (w - hi.astype(np.float32)).astype(jnp.bfloat16)
        out += [hi, lo]
    return out


def split(x):
    hi = x.astype(BF16)
    return hi, (x - hi.astype(F32)).astype(BF16)


def swap_tile(x):
    t = x.T
    return jnp.concatenate([t[32 * j:32 * j + 32] for j in range(4)], axis=1)


def fft16(re, im, sign):
    def four(a, b, c, d):
        (ar, ai), (br, bi), (cr, ci), (dr, di) = a, b, c, d
        sr, si, tr, ti = ar + cr, ai + ci, ar - cr, ai - ci
        ur, ui, vr, vi = br + dr, bi + di, br - dr, bi - di
        if sign < 0:
            wr, wi = vi, -vr
            return (sr + ur, si + ui), (tr + vi, ti - vr), (sr - ur, si - ui), (tr - vi, ti + vr)
        return (sr + ur, si + ui), (tr - vi, ti + vr), (sr - ur, si - ui), (tr + vi, ti - vr)

    x = list(zip(re, im))
    mid = [four(x[n], x[n + 4], x[n + 8], x[n + 12]) for n in range(4)]
    out = [None] * 16
    h = np.float32(math.sqrt(0.5))
    for k1 in range(4):
        col = []
        for n2 in range(4):
            zr, zi = mid[n2][k1]
            m = n2 * k1
            if m == 0:
                pass
            elif m == 4:
                zr, zi = (zi, -zr) if sign < 0 else (-zi, zr)
            elif m == 2:
                zr, zi = ((zr + zi) * h, (zi - zr) * h) if sign < 0 else ((zr - zi) * h, (zi + zr) * h)
            elif m == 6:
                zr, zi = ((zi - zr) * h, -(zr + zi) * h) if sign < 0 else (-(zr + zi) * h, (zr - zi) * h)
            else:
                c = np.float32(math.cos(2 * math.pi * m / 16))
                s = np.float32(sign * math.sin(2 * math.pi * m / 16))
                zr, zi = zr * c - zi * s, zr * s + zi * c
            col.append((zr, zi))
        res = four(*col)
        for k2 in range(4):
            out[k1 + 4 * k2] = res[k2]
    return [o[0] for o in out], [o[1] for o in out]


def own_tiles(x_ref):
    return [swap_tile(x_ref[0, :, LANES * t:LANES * t + LANES].astype(F32)) for t in range(8)]


def place_centre(tiles, cen):
    for t in range(8):
        for pair in range(4):
            cen[pl.ds(t * 128 + pair, 32, stride=4), :] = tiles[t]


def spectral_kernel(kern_ref, ksp, kdp):
    tiles = [swap_tile(kern_ref[:, LANES * t:LANES * t + LANES]) for t in range(8)]
    whole = jnp.concatenate(tiles, axis=0)

    def exact(a, f):
        one = a.astype(BF16)
        rest = a - one.astype(F32)
        two = rest.astype(BF16)
        three = (rest - two.astype(F32)).astype(BF16)
        return f(one) + (f(two) + f(three))
    row = lax.broadcasted_iota(jnp.int32, (LANES, LANES), 0)
    col = lax.broadcasted_iota(jnp.int32, (LANES, LANES), 1)
    mirror = jnp.bitwise_and(-jnp.bitwise_and(col, 96), 96) + jnp.bitwise_and(-col, 31)
    perm = jnp.where(row == mirror, 1.0, 0.0).astype(BF16)
    row = lax.broadcasted_iota(jnp.int32, (32, 32), 0)
    col = lax.broadcasted_iota(jnp.int32, (32, 32), 1)
    flip = jnp.where(row == jnp.bitwise_and(-col, 31), 1.0, 0.0).astype(BF16)
    lanes = exact(whole, lambda v: jnp.dot(v, perm, preferred_element_type=F32))
    rev = [lanes[32 * t:32 * t + 32] for t in range(8)]
    wide = jnp.concatenate(rev, axis=1)
    wide = exact(wide, lambda v: jnp.dot(flip, v, preferred_element_type=F32))
    rev = [wide[:, LANES * t:LANES * t + LANES] for t in range(8)]
    lane = lax.broadcasted_iota(jnp.int32, (32, LANES), 1)
    sym = []
    for t in range(8):
        other = jnp.where(lane < 32, rev[(8 - t) % 8], rev[7 - t])
        sym.append((tiles[t] + other) * np.float32(0.5))

    def groups(parts):
        out = None
        for g, (t, j) in enumerate(parts):
            v = sym[t]
            if (g - j) % 4:
                v = pltpu.roll(v, 32 * ((g - j) % 4), 1)
            out = v if out is None else jnp.where(lane >= 32 * g, v, out)
        return out
    scale = np.float32(2.0 / 32768)
    u0 = groups([(0, 0), (1, 0), (2, 0), (3, 0)])
    edge = pltpu.roll(sym[4], 16, 1)
    u0 = jnp.where((lane >= 16) & (lane < 32), edge, u0)
    u0 = u0 * scale
    half = np.float32(1.0 / 65536)
    first = sym[0]
    second = pltpu.roll(sym[0], LANES - 16, 1)
    third = sym[4]
    mean0, diff0 = (first + second) * half, (first - second) * half
    fourth = pltpu.roll(sym[4], LANES - 16, 1)
    mean1, diff1 = (third + fourth) * half, (third - fourth) * half
    mean1, diff1 = pltpu.roll(mean1, 16, 1), pltpu.roll(diff1, 16, 1)
    u0 = jnp.where(lane == 0, mean0, jnp.where(lane == 16, mean1, u0))
    d0 = jnp.where(lane == 0, diff0, jnp.where(lane == 16, diff1, jnp.zeros_like(diff0)))
    u1 = groups([(t, 2) for t in range(4)]) * scale
    u2 = groups([(t, 1) for t in range(4)]) * scale
    u3 = groups([(t + 4, 1) for t in range(4)]) * scale
    for pair in range(4):
        for u, v in enumerate((u0, u1, u2, u3)):
            ksp[pl.ds(u * 128 + pair, 16, stride=8), :] = v[:16]
            ksp[pl.ds(u * 128 + 4 + pair, 16, stride=8), :] = v[16:]
        kdp[pl.ds(pair, 16, stride=8), :] = d0[:16]
        kdp[pl.ds(4 + pair, 16, stride=8), :] = d0[16:]


def shift_boxes(pool, tab, zero_block, blocks, m):
    lane = lax.broadcasted_iota(jnp.int32, (8, LANES), 1)
    sub = lax.broadcasted_iota(jnp.int32, (8, LANES), 0)
    a_id = jnp.bitwise_and(lane, 31)
    b_id = sub * 4 + lax.shift_right_logical(lane, 5)

    def one(k, _):
        block, oc, ob, oa, use = tab(k)
        s = ob * 32 + oa
        r = jnp.bitwise_and(s, 127)
        sh = jnp.bitwise_and(lax.shift_right_arithmetic(s, 7), 7)
        lane_by = jnp.bitwise_and(128 - r, 127)
        sub_by = jnp.bitwise_and(8 - sh, 7)
        keep = (a_id + oa >= 0) & (a_id + oa < 32) & (b_id + ob >= 0) & (b_id + ob < 32)
        near = lane < 128 - r
        row = (k // 4) * 128 + k % 4
        for c in range(32):
            src = c + oc
            good = (src >= 0) & (src < 32) & use
            at = jnp.where(good, block + jnp.bitwise_and(src, 1) * blocks, zero_block)
            plane = jnp.where(good, lax.shift_right_arithmetic(src, 1), 0)
            v = pool[at, plane].astype(F32)
            v = pltpu.roll(v, lane_by, 1)
            v = pltpu.roll(v, sub_by, 0)
            w = pltpu.roll(v, 7, 0)
            v = jnp.where(keep, jnp.where(near, v, w), 0.0)
            m[pl.ds(row + 4 * c, 8, stride=MST), :] = v
        return 0
    lax.fori_loop(0, PAIRS, one, 0)


def densities(m, cen, yh, yl):
    def one(i, _):
        row = pl.multiple_of(i * 16, 16)
        crow = pl.multiple_of(jnp.bitwise_and(i, 7) * 16, 16)
        x = [m[pl.ds(pl.multiple_of(MST * t + row, 8), 16), :]
             * cen[pl.ds(pl.multiple_of(128 * t + crow, 16), 16), :] for t in range(8)]
        for h in range(2):
            e, o = x[h] + x[4 + h], x[2 + h] + x[6 + h]
            d, g = x[h] - x[4 + h], x[6 + h] - x[2 + h]
            for at, v in ((0, e + o), (256, e - o), (512, d), (768, g)):
                hi, lo = split(v)
                yh[pl.ds(row, 16), at + LANES * h:at + LANES * h + LANES] = hi
                yl[pl.ds(row, 16), at + LANES * h:at + LANES * h + LANES] = lo
        return 0
    lax.fori_loop(0, 24, one, 0)


CUTS = ((0, 256), (256, 512), (512, 1024))


def turn(yh, yl, w, s, back):
    for (b, e), (wh, wl) in zip(CUTS, w):
        hi, lo = yh[:, b:e], yl[:, b:e]
        dims = (((1,), (1 if back else 0,)), ((), ()))

        def dot(p, q):
            return lax.dot_general(p, q, dims, preferred_element_type=F32)
        out = dot(hi, wh[...]) + dot(lo, wh[...]) + dot(hi, wl[...])
        for t in range(b // LANES, e // LANES):
            s[t] = out[:, t * LANES - b:t * LANES - b + LANES]


def filtered(s, yh, yl, ksp, kdp):
    sub = lax.broadcasted_iota(jnp.int32, (8, LANES), 0)
    lower = sub < 4
    sgn = jnp.where(lower, np.float32(1), np.float32(-1))

    def twiddle(k):
        c = np.float32(math.cos(2 * math.pi * k / 32))
        n = np.float32(math.sin(2 * math.pi * k / 32))
        return jnp.where(lower, np.float32(1), c), jnp.where(lower, np.float32(0), n)

    def job(g, tr, ti, krow, special, energy):
        row = pl.multiple_of(g * 128, 128)
        re = [s[tr, pl.ds(row + 8 * n, 8), :] for n in range(16)]
        im = [s[ti, pl.ds(row + 8 * n, 8), :] for n in range(16)]
        re, im = fft16(re, im, -1)
        zr, zi = [], []
        for k in range(16):
            r, i = re[k], im[k]
            if k:
                c, n = twiddle(k)
                r, i = r * c + i * n, i * c - r * n
            zr.append(pltpu.roll(r, 4, 0) + sgn * r)
            zi.append(pltpu.roll(i, 4, 0) + sgn * i)
        wr, wi = [], []
        for k in range(16):
            km = ksp[pl.ds(krow + 8 * k, 8), :]
            r, i = zr[k] * km, zi[k] * km
            if special:
                kd = kdp[pl.ds(8 * k, 8), :]
                fr, fi = zr[(16 - k) % 16], zi[(16 - k) % 16]
                if k:
                    fr, fi = pltpu.roll(fr, 4, 0), pltpu.roll(fi, 4, 0)
                r, i = r + kd * fr, i - kd * fi
            energy = energy + (r * zr[k] + i * zi[k])
            wr.append(r)
            wi.append(i)
        re, im = [], []
        for k in range(16):
            r = pltpu.roll(wr[k], 4, 0) + sgn * wr[k]
            i = pltpu.roll(wi[k], 4, 0) + sgn * wi[k]
            if k:
                c, n = twiddle(k)
                r, i = r * c - i * n, i * c + r * n
            re.append(r)
            im.append(i)
        re, im = fft16(re, im, 1)
        for n in range(0, 16, 2):
            for t, z in ((tr, re), (ti, im)):
                hi, lo = split(jnp.concatenate([z[n], z[n + 1]], axis=0))
                at = pl.ds(row + 8 * n, 16)
                lanes = pl.ds(pl.multiple_of(t * LANES, LANES), LANES)
                yh[at, lanes] = hi
                yl[at, lanes] = lo
        return energy

    energy = jnp.zeros((8, LANES), F32)

    def first(g, e):
        return job(g, 0, 1, 0, True, e)

    def other(i, e):
        g, u = i // 3, i % 3 + 1
        tr = jnp.where(u == 1, 2, u + 2)
        ti = jnp.where(u == 1, 3, u + 4)
        return job(g, tr, ti, pl.multiple_of(u * 128, 128), False, e)
    energy = lax.fori_loop(0, GROUPS, first, energy)
    return lax.fori_loop(0, 3 * GROUPS, other, energy)


def collect(s, m, acc):
    def one(i, _):
        row = pl.multiple_of(i * 8, 8)
        for h in range(2):
            total = [None] * 4
            for g in range(GROUPS):
                y0, y2, yr, yi = (s[2 * n + h, pl.ds(g * 128 + row, 8), :] for n in range(4))
                p, q = y0 + y2, y0 - y2
                for n, v in enumerate((p + yr, q - yi, p - yr, q + yi)):
                    v = v * m[pl.ds(MST * (2 * n + h) + g * 128 + row, 8), :]
                    total[n] = v if total[n] is None else total[n] + v
            for n in range(4):
                acc[pl.ds((2 * n + h) * 128 + row, 8), :] = total[n]
        return 0
    lax.fori_loop(0, 16, one, 0)


def summed_tiles(acc):
    out = []
    for t in range(8):
        v = [acc[pl.ds(t * 128 + pair, 32, stride=4), :] for pair in range(4)]
        out.append((v[0] + v[1]) + (v[2] + v[3]))
    return out


HALO = 3
KEEP = {0: (0, 16), 1: (0, 16), 2: (0, 10), 3: (0, 4), -1: (0, 16), -2: (6, 10), -3: (12, 4)}
MESH = pl.DeviceIdType.MESH


def sign(v):
    return (v > 0) - (v < 0)


def routes(n_orb):
    out = []
    for core in range(2):
        tree = {}
        for dz in range(-HALO, HALO + 1):
            for dx in range(1 - n_orb // 2, n_orb // 2 + 1):
                if (dz, dx) == (0, 0):
                    continue
                way = sign(dx)
                if dx == n_orb // 2 and core == 1 and dz in (0, -1, -2):
                    way = -1
                if core == 0:
                    tree[dz, dx] = (sign(dz), 0) if dz else (0, way)
                else:
                    tree[dz, dx] = (0, way) if dx else (sign(dz), 0)
        out.append(tree)
    return out


def schedule(tree, core):
    def steps(p):
        dz, dx = p
        return (abs(dz) + abs(dx), abs(dx) if core == 0 else abs(dz), p)
    return sorted(tree, key=steps)


def kernel_body(n_slab, n_orb, x_ref, corners, partners, kern_hbm, *rest):
    w_hbm, rest = rest[:6], rest[6:]
    out_ref, en_ref = rest[:2]
    (pool, m, yh, yl, s, ksp, kdp, cen, acc, kern, part, other, echip, ex, ez) = rest[2:17]
    w_ref = rest[17:23]
    local_sem, send_sem, recv_sem, swap_send, swap_recv, tail_sem, ready_one, ready_two = rest[23:]
    here_x = lax.axis_index("orb")
    here_z = lax.axis_index("slab")
    rep = lax.axis_index("rep")
    blocks = (2 * HALO + 1) * n_orb
    zero_block = 2 * blocks

    loads = [pltpu.make_async_copy(kern_hbm, kern, local_sem.at[0])]
    loads += [pltpu.make_async_copy(a, b, local_sem.at[1 + i]) for i, (a, b) in enumerate(zip(w_hbm, w_ref))]
    for load in loads:
        load.start()

    def at_slab(step):
        return {"slab": lax.rem(here_z + step + n_slab, n_slab)}

    def at_orb(step):
        return {"orb": lax.rem(here_x + step + n_orb, n_orb)}
    sibling = {"rep": 1 - rep}

    barrier = pltpu.get_barrier_semaphore()
    for peer in (at_orb(1), at_orb(-1), at_slab(1), at_slab(-1), sibling):
        pl.semaphore_signal(barrier, inc=1, device_id=peer, device_id_type=MESH)

    tiles = own_tiles(x_ref)
    for t in range(8):
        acc[pl.ds(t, 32, stride=8), :] = tiles[t]
    own_block = HALO * n_orb + here_x
    mine = rep * blocks + own_block
    for c in range(16):
        even = acc[16 * c:16 * c + 8, :]
        odd = acc[16 * c + 8:16 * c + 16, :]
        pool[mine, c] = jnp.where(rep == 0, even, odd).astype(BF16)
    pool[zero_block, 0] = jnp.zeros((8, LANES), BF16)
    pl.semaphore_wait(barrier, 5)

    def slot(core, p):
        first, count = KEEP[p[0]]
        block = core * blocks + (p[0] + HALO) * n_orb + lax.rem(here_x + p[1] + n_orb, n_orb)
        return pool.at[block, pl.ds(first, count)]

    def index(p):
        return (p[0] + HALO) * n_orb + (p[1] + n_orb) % n_orb

    def swap(core, p):
        return pltpu.make_async_remote_copy(
            src_ref=slot(core, p), dst_ref=slot(core, p), send_sem=swap_send.at[index(p)],
            recv_sem=swap_recv.at[index(p)], device_id=sibling, device_id_type=MESH)

    def pass_on(core, p, hop):
        first, count = KEEP[p[0]]
        held = (p[0] - hop[0], p[1] - hop[1])
        x_slot = lax.rem(here_x + held[1] + n_orb, n_orb)
        src = pool.at[core * blocks + (held[0] + HALO) * n_orb + x_slot, pl.ds(first, count)]
        dst = pool.at[core * blocks + (p[0] + HALO) * n_orb + x_slot, pl.ds(first, count)]
        peer = at_slab(-hop[0]) if hop[0] else at_orb(-hop[1])
        return pltpu.make_async_remote_copy(
            src_ref=src, dst_ref=dst, send_sem=send_sem.at[index(p)], recv_sem=recv_sem.at[index(p)],
            device_id=peer, device_id_type=MESH)

    def arrival(core, p):
        return pltpu.make_async_remote_copy(
            src_ref=slot(core, p), dst_ref=slot(core, p), send_sem=send_sem.at[index(p)],
            recv_sem=recv_sem.at[index(p)], device_id=sibling, device_id_type=MESH)

    trees = routes(n_orb)

    def spread(core, held):
        for p, hop in trees[core].items():
            h = (p[0] - hop[0], p[1] - hop[1])
            if h == held or (h[0] == held[0] and (h[1] - held[1]) % n_orb == 0):
                pass_on(core, p, hop).start()
        swap(core, held).start()

    for core in range(2):
        @pl.when(rep == core)
        def _(core=core):
            spread(core, (0, 0))

    place_centre(tiles, cen)
    loads[0].wait()
    spectral_kernel(kern, ksp, kdp)

    for core in range(2):
        @pl.when(rep == core)
        def _(core=core):
            for p in schedule(trees[core], core):
                arrival(core, p).wait_recv()
                spread(core, p)
            for p in trees[core]:
                arrival(core, p).wait_send()
            for p in [(0, 0)] + list(trees[core]):
                swap(core, p).wait_send()
                swap(1 - core, p).wait_recv()

    def signal_far(sem):
        for step in (HALO, -HALO):
            pl.semaphore_signal(sem, inc=1, device_id=at_slab(step), device_id_type=MESH)
    signal_far(ready_one)

    own = here_z * n_orb + here_x

    def wrap(v):
        v = v + G // 2
        v = jnp.where(v < 0, v + G, jnp.where(v >= G, v - G, v))
        return v - G // 2

    def tab(k):
        j = partners[0, 2 * k + rep]
        use = j >= 0
        j = jnp.where(use, j, own)
        o = [wrap(corners[own, d] - corners[j, d]) for d in range(3)]
        dz = lax.div(j, n_orb) - here_z
        dz = jnp.where(dz > n_slab // 2, dz - n_slab, jnp.where(dz < -(n_slab // 2), dz + n_slab, dz))
        dz = jnp.clip(dz, -HALO, HALO)
        return (dz + HALO) * n_orb + lax.rem(j, n_orb), o[2], o[1], o[0], use

    shift_boxes(pool, tab, zero_block, blocks, m)
    densities(m, cen, yh, yl)
    for load in loads[1:]:
        load.wait()
    w = ((w_ref[0], w_ref[1]), (w_ref[2], w_ref[3]), (w_ref[4], w_ref[5]))
    pl.semaphore_wait(ready_one, 2)
    signal_far(ready_two)
    turn(yh, yl, w, s, False)
    energy = filtered(s, yh, yl, ksp, kdp)
    pl.semaphore_wait(ready_two, 2)

    echip[0] = jnp.sum(energy, axis=0, keepdims=True)
    swap_energy = pltpu.make_async_remote_copy(
        src_ref=echip.at[0], dst_ref=echip.at[1], send_sem=tail_sem.at[0], recv_sem=tail_sem.at[1],
        device_id=sibling, device_id_type=MESH)
    swap_energy.start()
    turn(yh, yl, w, s, True)
    swap_energy.wait()
    ex[here_x] = echip[0] + echip[1]

    def to_all(buf, here, size, at, sems):
        copies = []
        for step in range(1, size):
            copies.append(pltpu.make_async_remote_copy(
                src_ref=buf.at[here], dst_ref=buf.at[here], send_sem=sems[0].at[sems[1] + step],
                recv_sem=sems[0].at[sems[1] + size + step], device_id=at(step), device_id_type=MESH))
        return copies

    def from_all(buf, here, size, at, sems):
        for step in range(1, size):
            there = lax.rem(here - step + size, size)
            pltpu.make_async_remote_copy(
                src_ref=buf.at[there], dst_ref=buf.at[there], send_sem=sems[0].at[sems[1] + step],
                recv_sem=sems[0].at[sems[1] + size + step], device_id=at(step), device_id_type=MESH).wait_recv()
    x_sems = (tail_sem, 4)
    z_sems = (tail_sem, 4 + 2 * n_orb)
    x_copies = to_all(ex, here_x, n_orb, at_orb, x_sems)
    for copy in x_copies:
        copy.start()
    collect(s, m, acc)
    res = summed_tiles(acc)
    for t in range(8):
        part[t] = res[t]
    swap_part = pltpu.make_async_remote_copy(
        src_ref=part, dst_ref=other, send_sem=tail_sem.at[2], recv_sem=tail_sem.at[3],
        device_id=sibling, device_id_type=MESH)
    swap_part.start()
    from_all(ex, here_x, n_orb, at_orb, x_sems)
    ez[here_z] = functools.reduce(lambda a, b: a + b, [ex[i] for i in range(n_orb)])
    z_copies = to_all(ez, here_z, n_slab, at_slab, z_sems)
    for copy in z_copies:
        copy.start()
    swap_part.wait()
    for t in range(8):
        out_ref[0, :, LANES * t:LANES * t + LANES] = -swap_tile(part[t] + other[t])
    for copy in x_copies:
        copy.wait_send()
    from_all(ez, here_z, n_slab, at_slab, z_sems)
    total = functools.reduce(lambda a, b: a + b, [ez[i] for i in range(n_slab)])
    for copy in z_copies:
        copy.wait_send()
    en_ref[0] = jnp.sum(total) * np.float32(-1.0 / (2.0 * n_slab * n_orb * B ** 3))


def body(n_slab, n_orb, orbitals, corners, partners, kernel):
    blocks = (2 * HALO + 1) * n_orb
    vmem = pl.BlockSpec(memory_space=pltpu.VMEM)
    smem = pl.BlockSpec(memory_space=pltpu.SMEM)
    hbm = pl.BlockSpec(memory_space=pl.ANY)
    dma = pltpu.SemaphoreType.DMA
    weights = [jnp.asarray(w) for w in plane_tables()]
    return pl.pallas_call(
        functools.partial(kernel_body, n_slab, n_orb),
        out_shape=(jax.ShapeDtypeStruct((1, B, B * B), F32), jax.ShapeDtypeStruct((1,), F32)),
        in_specs=[vmem, smem, smem, hbm] + [hbm] * 6,
        out_specs=(vmem, smem),
        scratch_shapes=[
            pltpu.VMEM((2 * blocks + 1, 16, 8, LANES), BF16),
            pltpu.VMEM((8 * MST, LANES), F32),
            pltpu.VMEM((384, 1024), BF16),
            pltpu.VMEM((384, 1024), BF16),
            pltpu.VMEM((8, 384, LANES), F32),
            pltpu.VMEM((512, LANES), F32),
            pltpu.VMEM((128, LANES), F32),
            pltpu.VMEM((1024, LANES), F32),
            pltpu.VMEM((1024, LANES), F32),
            pltpu.VMEM((B, B * B), F32),
            pltpu.VMEM((8, B, LANES), F32),
            pltpu.VMEM((8, B, LANES), F32),
            pltpu.VMEM((2, 1, LANES), F32),
            pltpu.VMEM((n_orb, 1, LANES), F32),
            pltpu.VMEM((n_slab, 1, LANES), F32),
            *[pltpu.VMEM(w.shape, BF16) for w in weights],
            dma((7,)),
            dma((blocks,)),
            dma((blocks,)),
            dma((blocks,)),
            dma((blocks,)),
            dma((4 + 2 * n_orb + 2 * n_slab,)),
            pltpu.SemaphoreType.REGULAR,
            pltpu.SemaphoreType.REGULAR,
        ],
        compiler_params=pltpu.CompilerParams(
            collective_id=0, has_side_effects=True, vmem_limit_bytes=67043328),
    )(orbitals, corners, partners, kernel, *weights)


def solution(mesh):
    in_specs = (
        P(("grp", "slab", "orb"), None, None),
        P("grp", None),
        P(("grp", "slab", "orb"), None),
        P(),
    )
    out_specs = (P(("grp", "slab", "orb"), None, None), P("grp"))
    step = functools.partial(body, mesh.shape["slab"], mesh.shape["orb"])
    return jax.shard_map(step, mesh=mesh, in_specs=in_specs, out_specs=out_specs, check_vma=False)
```

```python
import functools, math
import jax, jax.numpy as jnp, numpy as np
from jax import lax
from jax.experimental import pallas as pl
from jax.sharding import PartitionSpec as P
from jax.experimental.pallas import tpu as pltpu

G = 192
ZDEV = 12
B = 32
LANES = 128
PAIRS = 12
GROUPS = 3
MST = 392
F32 = jnp.float32
BF16 = jnp.bfloat16


def plane_tables():
    def th(q, p, bl, a):
        return 2 * np.pi * ((q * bl + p * a) % 32) / 32
    bl = np.repeat(np.arange(8), 32)[:, None]
    a = np.tile(np.arange(32), 8)[:, None]
    lane = np.arange(128)
    g, r = lane // 32, lane % 32
    q = np.where(g > 0, 4 * g, np.where(r < 16, 0, 16))
    p = np.where(g > 0, r, r % 16)
    t = th(q, p, bl, a)
    w0 = np.concatenate([np.cos(t), -np.sin(t)], 1)
    for l in (0, 16):
        w0[:, 128 + l] = np.cos(th(q[l], 16, bl, a))[:, 0]
    t = th(2 + 4 * g, r, bl, a)
    w2 = np.concatenate([np.cos(t), -np.sin(t)], 1)
    l2 = np.arange(256)
    t = th(1 + 4 * (l2 // 32), l2 % 32, bl, a)
    c, s = np.cos(t), np.sin(t)
    w1 = np.block([[c, -s], [s, c]])
    out = []
    for w in (w0, w2, w1):
        w = w.astype(np.float32)
        hi = w.astype(jnp.bfloat16)
        lo = (w - hi.astype(np.float32)).astype(jnp.bfloat16)
        out += [hi, lo]
    return out


def split(x):
    hi = x.astype(BF16)
    return hi, (x - hi.astype(F32)).astype(BF16)


def swap_tile(x):
    t = x.T
    return jnp.concatenate([t[32 * j:32 * j + 32] for j in range(4)], axis=1)


def fft16(re, im, sign):
    def four(a, b, c, d):
        (ar, ai), (br, bi), (cr, ci), (dr, di) = a, b, c, d
        sr, si, tr, ti = ar + cr, ai + ci, ar - cr, ai - ci
        ur, ui, vr, vi = br + dr, bi + di, br - dr, bi - di
        if sign < 0:
            wr, wi = vi, -vr
            return (sr + ur, si + ui), (tr + vi, ti - vr), (sr - ur, si - ui), (tr - vi, ti + vr)
        return (sr + ur, si + ui), (tr - vi, ti + vr), (sr - ur, si - ui), (tr + vi, ti - vr)

    x = list(zip(re, im))
    mid = [four(x[n], x[n + 4], x[n + 8], x[n + 12]) for n in range(4)]
    out = [None] * 16
    h = np.float32(math.sqrt(0.5))
    for k1 in range(4):
        col = []
        for n2 in range(4):
            zr, zi = mid[n2][k1]
            m = n2 * k1
            if m == 0:
                pass
            elif m == 4:
                zr, zi = (zi, -zr) if sign < 0 else (-zi, zr)
            elif m == 2:
                zr, zi = ((zr + zi) * h, (zi - zr) * h) if sign < 0 else ((zr - zi) * h, (zi + zr) * h)
            elif m == 6:
                zr, zi = ((zi - zr) * h, -(zr + zi) * h) if sign < 0 else (-(zr + zi) * h, (zr - zi) * h)
            else:
                c = np.float32(math.cos(2 * math.pi * m / 16))
                s = np.float32(sign * math.sin(2 * math.pi * m / 16))
                zr, zi = zr * c - zi * s, zr * s + zi * c
            col.append((zr, zi))
        res = four(*col)
        for k2 in range(4):
            out[k1 + 4 * k2] = res[k2]
    return [o[0] for o in out], [o[1] for o in out]


def own_tiles(x_ref):
    return [swap_tile(x_ref[0, :, LANES * t:LANES * t + LANES].astype(F32)) for t in range(8)]


def place_centre(tiles, cen):
    for t in range(8):
        for pair in range(4):
            cen[pl.ds(t * 128 + pair, 32, stride=4), :] = tiles[t]


def spectral_kernel(kern_ref, ksp, kdp):
    tiles = [swap_tile(kern_ref[:, LANES * t:LANES * t + LANES]) for t in range(8)]
    whole = jnp.concatenate(tiles, axis=0)

    def exact(a, f):
        one = a.astype(BF16)
        rest = a - one.astype(F32)
        two = rest.astype(BF16)
        three = (rest - two.astype(F32)).astype(BF16)
        return f(one) + (f(two) + f(three))
    row = lax.broadcasted_iota(jnp.int32, (LANES, LANES), 0)
    col = lax.broadcasted_iota(jnp.int32, (LANES, LANES), 1)
    mirror = jnp.bitwise_and(-jnp.bitwise_and(col, 96), 96) + jnp.bitwise_and(-col, 31)
    perm = jnp.where(row == mirror, 1.0, 0.0).astype(BF16)
    row = lax.broadcasted_iota(jnp.int32, (32, 32), 0)
    col = lax.broadcasted_iota(jnp.int32, (32, 32), 1)
    flip = jnp.where(row == jnp.bitwise_and(-col, 31), 1.0, 0.0).astype(BF16)
    lanes = exact(whole, lambda v: jnp.dot(v, perm, preferred_element_type=F32))
    rev = [lanes[32 * t:32 * t + 32] for t in range(8)]
    wide = jnp.concatenate(rev, axis=1)
    wide = exact(wide, lambda v: jnp.dot(flip, v, preferred_element_type=F32))
    rev = [wide[:, LANES * t:LANES * t + LANES] for t in range(8)]
    lane = lax.broadcasted_iota(jnp.int32, (32, LANES), 1)
    sym = []
    for t in range(8):
        other = jnp.where(lane < 32, rev[(8 - t) % 8], rev[7 - t])
        sym.append((tiles[t] + other) * np.float32(0.5))

    def groups(parts):
        out = None
        for g, (t, j) in enumerate(parts):
            v = sym[t]
            if (g - j) % 4:
                v = pltpu.roll(v, 32 * ((g - j) % 4), 1)
            out = v if out is None else jnp.where(lane >= 32 * g, v, out)
        return out
    scale = np.float32(2.0 / 32768)
    u0 = groups([(0, 0), (1, 0), (2, 0), (3, 0)])
    edge = pltpu.roll(sym[4], 16, 1)
    u0 = jnp.where((lane >= 16) & (lane < 32), edge, u0)
    u0 = u0 * scale
    half = np.float32(1.0 / 65536)
    first = sym[0]
    second = pltpu.roll(sym[0], LANES - 16, 1)
    third = sym[4]
    mean0, diff0 = (first + second) * half, (first - second) * half
    fourth = pltpu.roll(sym[4], LANES - 16, 1)
    mean1, diff1 = (third + fourth) * half, (third - fourth) * half
    mean1, diff1 = pltpu.roll(mean1, 16, 1), pltpu.roll(diff1, 16, 1)
    u0 = jnp.where(lane == 0, mean0, jnp.where(lane == 16, mean1, u0))
    d0 = jnp.where(lane == 0, diff0, jnp.where(lane == 16, diff1, jnp.zeros_like(diff0)))
    u1 = groups([(t, 2) for t in range(4)]) * scale
    u2 = groups([(t, 1) for t in range(4)]) * scale
    u3 = groups([(t + 4, 1) for t in range(4)]) * scale
    for pair in range(4):
        for u, v in enumerate((u0, u1, u2, u3)):
            ksp[pl.ds(u * 128 + pair, 16, stride=8), :] = v[:16]
            ksp[pl.ds(u * 128 + 4 + pair, 16, stride=8), :] = v[16:]
        kdp[pl.ds(pair, 16, stride=8), :] = d0[:16]
        kdp[pl.ds(4 + pair, 16, stride=8), :] = d0[16:]


def shift_boxes(pool, tab, zero_block, blocks, m):
    lane = lax.broadcasted_iota(jnp.int32, (8, LANES), 1)
    sub = lax.broadcasted_iota(jnp.int32, (8, LANES), 0)
    a_id = jnp.bitwise_and(lane, 31)
    b_id = sub * 4 + lax.shift_right_logical(lane, 5)

    def one(k, _):
        block, oc, ob, oa, use = tab(k)
        s = ob * 32 + oa
        r = jnp.bitwise_and(s, 127)
        sh = jnp.bitwise_and(lax.shift_right_arithmetic(s, 7), 7)
        lane_by = jnp.bitwise_and(128 - r, 127)
        sub_by = jnp.bitwise_and(8 - sh, 7)
        keep = (a_id + oa >= 0) & (a_id + oa < 32) & (b_id + ob >= 0) & (b_id + ob < 32)
        near = lane < 128 - r
        row = (k // 4) * 128 + k % 4
        for c in range(32):
            src = c + oc
            good = (src >= 0) & (src < 32) & use
            at = jnp.where(good, block + jnp.bitwise_and(src, 1) * blocks, zero_block)
            plane = jnp.where(good, lax.shift_right_arithmetic(src, 1), 0)
            v = pool[at, plane].astype(F32)
            v = pltpu.roll(v, lane_by, 1)
            v = pltpu.roll(v, sub_by, 0)
            w = pltpu.roll(v, 7, 0)
            v = jnp.where(keep, jnp.where(near, v, w), 0.0)
            m[pl.ds(row + 4 * c, 8, stride=MST), :] = v
        return 0
    lax.fori_loop(0, PAIRS, one, 0)


def densities(m, cen, yh, yl):
    def one(i, _):
        row = pl.multiple_of(i * 16, 16)
        crow = pl.multiple_of(jnp.bitwise_and(i, 7) * 16, 16)
        x = [m[pl.ds(pl.multiple_of(MST * t + row, 8), 16), :]
             * cen[pl.ds(pl.multiple_of(128 * t + crow, 16), 16), :] for t in range(8)]
        for h in range(2):
            e, o = x[h] + x[4 + h], x[2 + h] + x[6 + h]
            d, g = x[h] - x[4 + h], x[6 + h] - x[2 + h]
            for at, v in ((0, e + o), (256, e - o), (512, d), (768, g)):
                hi, lo = split(v)
                yh[pl.ds(row, 16), at + LANES * h:at + LANES * h + LANES] = hi
                yl[pl.ds(row, 16), at + LANES * h:at + LANES * h + LANES] = lo
        return 0
    lax.fori_loop(0, 24, one, 0)


CUTS = ((0, 256), (256, 512), (512, 1024))


def turn(yh, yl, w, s, back):
    for (b, e), (wh, wl) in zip(CUTS, w):
        hi, lo = yh[:, b:e], yl[:, b:e]
        dims = (((1,), (1 if back else 0,)), ((), ()))

        def dot(p, q):
            return lax.dot_general(p, q, dims, preferred_element_type=F32)
        out = dot(hi, wh[...]) + dot(lo, wh[...]) + dot(hi, wl[...])
        for t in range(b // LANES, e // LANES):
            s[t] = out[:, t * LANES - b:t * LANES - b + LANES]


def filtered(s, yh, yl, ksp, kdp):
    sub = lax.broadcasted_iota(jnp.int32, (8, LANES), 0)
    lower = sub < 4
    sgn = jnp.where(lower, np.float32(1), np.float32(-1))

    def twiddle(k):
        c = np.float32(math.cos(2 * math.pi * k / 32))
        n = np.float32(math.sin(2 * math.pi * k / 32))
        return jnp.where(lower, np.float32(1), c), jnp.where(lower, np.float32(0), n)

    def job(g, tr, ti, krow, special, energy):
        row = pl.multiple_of(g * 128, 128)
        re = [s[tr, pl.ds(row + 8 * n, 8), :] for n in range(16)]
        im = [s[ti, pl.ds(row + 8 * n, 8), :] for n in range(16)]
        re, im = fft16(re, im, -1)
        zr, zi = [], []
        for k in range(16):
            r, i = re[k], im[k]
            if k:
                c, n = twiddle(k)
                r, i = r * c + i * n, i * c - r * n
            zr.append(pltpu.roll(r, 4, 0) + sgn * r)
            zi.append(pltpu.roll(i, 4, 0) + sgn * i)
        wr, wi = [], []
        for k in range(16):
            km = ksp[pl.ds(krow + 8 * k, 8), :]
            r, i = zr[k] * km, zi[k] * km
            if special:
                kd = kdp[pl.ds(8 * k, 8), :]
                fr, fi = zr[(16 - k) % 16], zi[(16 - k) % 16]
                if k:
                    fr, fi = pltpu.roll(fr, 4, 0), pltpu.roll(fi, 4, 0)
                r, i = r + kd * fr, i - kd * fi
            energy = energy + (r * zr[k] + i * zi[k])
            wr.append(r)
            wi.append(i)
        re, im = [], []
        for k in range(16):
            r = pltpu.roll(wr[k], 4, 0) + sgn * wr[k]
            i = pltpu.roll(wi[k], 4, 0) + sgn * wi[k]
            if k:
                c, n = twiddle(k)
                r, i = r * c - i * n, i * c + r * n
            re.append(r)
            im.append(i)
        re, im = fft16(re, im, 1)
        for n in range(0, 16, 2):
            for t, z in ((tr, re), (ti, im)):
                hi, lo = split(jnp.concatenate([z[n], z[n + 1]], axis=0))
                at = pl.ds(row + 8 * n, 16)
                lanes = pl.ds(pl.multiple_of(t * LANES, LANES), LANES)
                yh[at, lanes] = hi
                yl[at, lanes] = lo
        return energy

    energy = jnp.zeros((8, LANES), F32)

    def first(g, e):
        return job(g, 0, 1, 0, True, e)

    def other(i, e):
        g, u = i // 3, i % 3 + 1
        tr = jnp.where(u == 1, 2, u + 2)
        ti = jnp.where(u == 1, 3, u + 4)
        return job(g, tr, ti, pl.multiple_of(u * 128, 128), False, e)
    energy = lax.fori_loop(0, GROUPS, first, energy)
    return lax.fori_loop(0, 3 * GROUPS, other, energy)


def collect(s, m, acc):
    def one(i, _):
        row = pl.multiple_of(i * 8, 8)
        for h in range(2):
            total = [None] * 4
            for g in range(GROUPS):
                y0, y2, yr, yi = (s[2 * n + h, pl.ds(g * 128 + row, 8), :] for n in range(4))
                p, q = y0 + y2, y0 - y2
                for n, v in enumerate((p + yr, q - yi, p - yr, q + yi)):
                    v = v * m[pl.ds(MST * (2 * n + h) + g * 128 + row, 8), :]
                    total[n] = v if total[n] is None else total[n] + v
            for n in range(4):
                acc[pl.ds((2 * n + h) * 128 + row, 8), :] = total[n]
        return 0
    lax.fori_loop(0, 16, one, 0)


def summed_tiles(acc):
    out = []
    for t in range(8):
        v = [acc[pl.ds(t * 128 + pair, 32, stride=4), :] for pair in range(4)]
        out.append((v[0] + v[1]) + (v[2] + v[3]))
    return out


HALO = 3
KEEP = (
    {0: (0, 16), 1: (0, 16), 2: (0, 10), 3: (0, 4), -1: (1, 15), -2: (7, 9), -3: (13, 3)},
    {0: (0, 16), 1: (0, 15), 2: (0, 9), 3: (0, 3), -1: (0, 16), -2: (6, 10), -3: (12, 4)},
)
MESH = pl.DeviceIdType.MESH


def sign(v):
    return (v > 0) - (v < 0)


ORB_HOP = {1: 1, 2: 2, 3: 3, 4: 4}
SLAB_HOP = {1: 1, 2: 2, 3: 3}
LATE_HOP = {1: 1, 2: 1, 3: 1, 4: 1}


def routes(n_orb):
    out = []
    for core in range(2):
        tree = {}
        for dz in range(-HALO, HALO + 1):
            for dx in range(1 - n_orb // 2, n_orb // 2 + 1):
                if (dz, dx) == (0, 0):
                    continue
                way = sign(dx)
                if dx == n_orb // 2 and core == 1 and dz in (0, -1, -2):
                    way = -1
                if core == 0:
                    tree[dz, dx] = (sign(dz) * SLAB_HOP[abs(dz)], 0) if dz else (0, way * ORB_HOP[abs(dx)])
                else:
                    tree[dz, dx] = (0, way * LATE_HOP[abs(dx)]) if dx else (sign(dz) * SLAB_HOP[abs(dz)], 0)
        out.append(tree)
    return out


def held_as(tree, p, n_orb):
    dz, dx = p[0] - tree[p][0], p[1] - tree[p][1]
    return dz, (dx + n_orb // 2 - 1) % n_orb - n_orb // 2 + 1


def schedule(tree, n_orb):
    def depth(p):
        return 0 if p == (0, 0) else 1 + depth(held_as(tree, p, n_orb))
    return sorted(tree, key=lambda p: (depth(p), abs(p[0]) + abs(p[1]), p))


def kernel_body(n_slab, n_orb, x_hbm, corners_hbm, partners_hbm, kern_hbm, *rest):
    w_hbm, rest = rest[:6], rest[6:]
    out_ref, en_ref = rest[:2]
    (pool, m, yh, yl, s, ksp, kdp, cen, acc, kern, part, other, ex, ez) = rest[2:16]
    w_ref = rest[16:22]
    x_ref, corners, partners = rest[22:25]
    local_sem, send_sem, recv_sem, swap_send, swap_recv, tail_sem, ready_one, ready_two = rest[25:]
    here_x = lax.axis_index("orb")
    here_z = lax.axis_index("slab")
    rep = lax.axis_index("rep")
    blocks = (2 * HALO + 1) * n_orb
    zero_block = 2 * blocks

    def at_slab(step):
        return {"slab": lax.rem(here_z + step + n_slab, n_slab)}

    def at_orb(step):
        return {"orb": lax.rem(here_x + step + n_orb, n_orb)}
    sibling = {"rep": 1 - rep}

    trees = routes(n_orb)

    def at(hop):
        return {**at_slab(hop[0]), **at_orb(hop[1])}
    barrier = pltpu.get_barrier_semaphore()
    pl.semaphore_signal(barrier, inc=1, device_id=sibling, device_id_type=MESH)
    for core in range(2):
        @pl.when(rep == core)
        def _(core=core):
            for hop in sorted(set(trees[core].values())):
                pl.semaphore_signal(barrier, inc=1, device_id=at(hop), device_id_type=MESH)

    x_load = pltpu.make_async_copy(x_hbm, x_ref, local_sem.at[0])
    x_load.start()
    loads = [pltpu.make_async_copy(a, b, local_sem.at[1 + i]) for i, (a, b) in enumerate(zip(
        (kern_hbm, corners_hbm, partners_hbm) + w_hbm, (kern, corners, partners) + w_ref))]
    for load in loads:
        load.start()
    x_load.wait()
    tiles = own_tiles(x_ref)
    for t in range(8):
        acc[pl.ds(t, 32, stride=8), :] = tiles[t]
    own_block = HALO * n_orb + here_x
    mine = rep * blocks + own_block
    for c in range(16):
        even = acc[16 * c:16 * c + 8, :]
        odd = acc[16 * c + 8:16 * c + 16, :]
        pool[mine, c] = jnp.where(rep == 0, even, odd).astype(BF16)
    pool[zero_block, 0] = jnp.zeros((8, LANES), BF16)
    for core in range(2):
        @pl.when(rep == core)
        def _(core=core):
            pl.semaphore_wait(barrier, len(set(trees[core].values())) + 1)

    def signal_far(sem):
        for step in (HALO, -HALO):
            pl.semaphore_signal(sem, inc=1, device_id=at_slab(step), device_id_type=MESH)

    def slot(core, p):
        first, count = KEEP[core][p[0]]
        block = core * blocks + (p[0] + HALO) * n_orb + lax.rem(here_x + p[1] + n_orb, n_orb)
        return pool.at[block, pl.ds(first, count)]

    def index(p):
        return (p[0] + HALO) * n_orb + (p[1] + n_orb) % n_orb

    def swap(core, p):
        return pltpu.make_async_remote_copy(
            src_ref=slot(core, p), dst_ref=slot(core, p), send_sem=swap_send.at[index(p)],
            recv_sem=swap_recv.at[index(p)], device_id=sibling, device_id_type=MESH)

    def pass_on(core, p, hop):
        first, count = KEEP[core][p[0]]
        held = (p[0] - hop[0], p[1] - hop[1])
        x_slot = lax.rem(here_x + held[1] + n_orb, n_orb)
        src = pool.at[core * blocks + (held[0] + HALO) * n_orb + x_slot, pl.ds(first, count)]
        dst = pool.at[core * blocks + (p[0] + HALO) * n_orb + x_slot, pl.ds(first, count)]
        peer = at((-hop[0], -hop[1]))
        return pltpu.make_async_remote_copy(
            src_ref=src, dst_ref=dst, send_sem=send_sem.at[index(p)], recv_sem=recv_sem.at[index(p)],
            device_id=peer, device_id_type=MESH)

    def arrival(core, p):
        return pltpu.make_async_remote_copy(
            src_ref=slot(core, p), dst_ref=slot(core, p), send_sem=send_sem.at[index(p)],
            recv_sem=recv_sem.at[index(p)], device_id=sibling, device_id_type=MESH)

    def spread(core, held):
        tree = trees[core]
        for p in sorted(tree, key=lambda p: -abs(tree[p][0]) - abs(tree[p][1])):
            if held_as(tree, p, n_orb) == held:
                pass_on(core, p, tree[p]).start()
        swap(core, held).start()

    for core in range(2):
        @pl.when(rep == core)
        def _(core=core):
            spread(core, (0, 0))

    signal_far(ready_one)
    place_centre(tiles, cen)
    loads[0].wait()
    spectral_kernel(kern, ksp, kdp)

    for core in range(2):
        @pl.when(rep == core)
        def _(core=core):
            for p in schedule(trees[core], n_orb):
                arrival(core, p).wait_recv()
                spread(core, p)
            for p in trees[core]:
                arrival(core, p).wait_send()
            for p in [(0, 0)] + list(trees[core]):
                swap(core, p).wait_send()
                swap(1 - core, p).wait_recv()

    pl.semaphore_wait(ready_one, 2)
    signal_far(ready_two)

    own = here_z * n_orb + here_x

    def wrap(v):
        v = v + G // 2
        v = jnp.where(v < 0, v + G, jnp.where(v >= G, v - G, v))
        return v - G // 2

    loads[1].wait()
    loads[2].wait()

    def tab(k):
        j = partners[0, 2 * k + rep]
        use = j >= 0
        j = jnp.where(use, j, own)
        o = [wrap(corners[own, d] - corners[j, d]) for d in range(3)]
        dz = lax.div(j, n_orb) - here_z
        dz = jnp.where(dz > n_slab // 2, dz - n_slab, jnp.where(dz < -(n_slab // 2), dz + n_slab, dz))
        dz = jnp.clip(dz, -HALO, HALO)
        return (dz + HALO) * n_orb + lax.rem(j, n_orb), o[2], o[1], o[0], use

    shift_boxes(pool, tab, zero_block, blocks, m)
    densities(m, cen, yh, yl)
    for load in loads[3:]:
        load.wait()
    w = ((w_ref[0], w_ref[1]), (w_ref[2], w_ref[3]), (w_ref[4], w_ref[5]))
    turn(yh, yl, w, s, False)
    energy = filtered(s, yh, yl, ksp, kdp)
    pl.semaphore_wait(ready_two, 2)

    me = 2 * here_x + rep
    ex[me] = jnp.sum(energy, axis=0, keepdims=True)

    def to_slab(step, cross, back):
        other_rep = 1 - rep if cross else rep
        there = 2 * lax.rem(here_x - step + n_orb, n_orb) + other_rep
        cell = ex.at[there if back else me]
        n = 2 * step + cross
        return pltpu.make_async_remote_copy(
            src_ref=cell, dst_ref=cell, send_sem=tail_sem.at[2 + n], recv_sem=tail_sem.at[2 + 2 * n_orb + n],
            device_id={**at_orb(step), "rep": other_rep}, device_id_type=MESH)

    def to_column(step, back):
        cell = ez.at[lax.rem(here_z - step + n_slab, n_slab) if back else here_z]
        first = 2 + 4 * n_orb
        return pltpu.make_async_remote_copy(
            src_ref=cell, dst_ref=cell, send_sem=tail_sem.at[first + step],
            recv_sem=tail_sem.at[first + n_slab + step], device_id=at_slab(step), device_id_type=MESH)
    near = [(step, cross) for step in range(n_orb) for cross in range(2) if step or cross]
    near.sort(key=lambda v: -min(v[0], n_orb - v[0]))
    far = sorted(range(1, n_slab), key=lambda v: -min(v, n_slab - v))
    for step, cross in near:
        to_slab(step, cross, False).start()
    turn(yh, yl, w, s, True)
    collect(s, m, acc)
    res = summed_tiles(acc)
    for t in range(8):
        part[t] = res[t]
    swap_part = pltpu.make_async_remote_copy(
        src_ref=part, dst_ref=other, send_sem=tail_sem.at[0], recv_sem=tail_sem.at[1],
        device_id=sibling, device_id_type=MESH)
    swap_part.start()
    for step, cross in near:
        to_slab(step, cross, True).wait_recv()
    ez[here_z] = functools.reduce(lambda a, b: a + b, [ex[i] for i in range(2 * n_orb)])
    for step in far:
        to_column(step, False).start()
    swap_part.wait()
    for t in range(8):
        out_ref[0, :, LANES * t:LANES * t + LANES] = -swap_tile(part[t] + other[t])
    for step, cross in near:
        to_slab(step, cross, False).wait_send()
    for step in far:
        to_column(step, True).wait_recv()
    total = functools.reduce(lambda a, b: a + b, [ez[i] for i in range(n_slab)])
    for step in far:
        to_column(step, False).wait_send()
    en_ref[0] = jnp.sum(total) * np.float32(-1.0 / (2.0 * n_slab * n_orb * B ** 3))


def body(n_slab, n_orb, orbitals, corners, partners, kernel):
    blocks = (2 * HALO + 1) * n_orb
    vmem = pl.BlockSpec(memory_space=pltpu.VMEM)
    smem = pl.BlockSpec(memory_space=pltpu.SMEM)
    hbm = pl.BlockSpec(memory_space=pl.ANY)
    dma = pltpu.SemaphoreType.DMA
    weights = [jnp.asarray(w) for w in plane_tables()]
    return pl.pallas_call(
        functools.partial(kernel_body, n_slab, n_orb),
        out_shape=(jax.ShapeDtypeStruct((1, B, B * B), F32), jax.ShapeDtypeStruct((1,), F32)),
        in_specs=[hbm] * 10,
        out_specs=(vmem, smem),
        scratch_shapes=[
            pltpu.VMEM((2 * blocks + 1, 16, 8, LANES), BF16),
            pltpu.VMEM((8 * MST, LANES), F32),
            pltpu.VMEM((384, 1024), BF16),
            pltpu.VMEM((384, 1024), BF16),
            pltpu.VMEM((8, 384, LANES), F32),
            pltpu.VMEM((512, LANES), F32),
            pltpu.VMEM((128, LANES), F32),
            pltpu.VMEM((1024, LANES), F32),
            pltpu.VMEM((1024, LANES), F32),
            pltpu.VMEM((B, B * B), F32),
            pltpu.VMEM((8, B, LANES), F32),
            pltpu.VMEM((8, B, LANES), F32),
            pltpu.VMEM((2 * n_orb, 1, LANES), F32),
            pltpu.VMEM((n_slab, 1, LANES), F32),
            *[pltpu.VMEM(w.shape, BF16) for w in weights],
            pltpu.VMEM((1, B, B * B), BF16),
            pltpu.SMEM(corners.shape, jnp.int32),
            pltpu.SMEM(partners.shape, jnp.int32),
            dma((10,)),
            dma((blocks,)),
            dma((blocks,)),
            dma((blocks,)),
            dma((blocks,)),
            dma((2 + 4 * n_orb + 2 * n_slab,)),
            pltpu.SemaphoreType.REGULAR,
            pltpu.SemaphoreType.REGULAR,
        ],
        compiler_params=pltpu.CompilerParams(
            collective_id=0, has_side_effects=True, vmem_limit_bytes=67043328),
    )(orbitals, corners, partners, kernel, *weights)


def solution(mesh):
    in_specs = (
        P(("grp", "slab", "orb"), None, None),
        P("grp", None),
        P(("grp", "slab", "orb"), None),
        P(),
    )
    out_specs = (P(("grp", "slab", "orb"), None, None), P("grp"))
    step = functools.partial(body, mesh.shape["slab"], mesh.shape["orb"])
    return jax.shard_map(step, mesh=mesh, in_specs=in_specs, out_specs=out_specs, check_vma=False)
```

```python
import functools, math
import jax, jax.numpy as jnp, numpy as np
from jax import lax
from jax.experimental import pallas as pl
from jax.sharding import PartitionSpec as P
from jax.experimental.pallas import tpu as pltpu

G = 192
ZDEV = 12
B = 32
LANES = 128
PAIRS = 12
GROUPS = 3
MST = 392
F32 = jnp.float32
BF16 = jnp.bfloat16


def plane_tables():
    def th(q, p, bl, a):
        return 2 * np.pi * ((q * bl + p * a) % 32) / 32
    bl = np.repeat(np.arange(8), 32)[:, None]
    a = np.tile(np.arange(32), 8)[:, None]
    lane = np.arange(128)
    g, r = lane // 32, lane % 32
    q = np.where(g > 0, 4 * g, np.where(r < 16, 0, 16))
    p = np.where(g > 0, r, r % 16)
    t = th(q, p, bl, a)
    w0 = np.concatenate([np.cos(t), -np.sin(t)], 1)
    for l in (0, 16):
        w0[:, 128 + l] = np.cos(th(q[l], 16, bl, a))[:, 0]
    t = th(2 + 4 * g, r, bl, a)
    w2 = np.concatenate([np.cos(t), -np.sin(t)], 1)
    l2 = np.arange(256)
    t = th(1 + 4 * (l2 // 32), l2 % 32, bl, a)
    c, s = np.cos(t), np.sin(t)
    w1 = np.block([[c, -s], [s, c]])
    out = []
    for w in (w0, w2, w1):
        w = w.astype(np.float32)
        hi = w.astype(jnp.bfloat16)
        lo = (w - hi.astype(np.float32)).astype(jnp.bfloat16)
        out += [hi, lo]
    return out


def split(x):
    hi = x.astype(BF16)
    return hi, (x - hi.astype(F32)).astype(BF16)


def swap_tile(x):
    t = x.T
    return jnp.concatenate([t[32 * j:32 * j + 32] for j in range(4)], axis=1)


def fft16(re, im, sign):
    def four(a, b, c, d):
        (ar, ai), (br, bi), (cr, ci), (dr, di) = a, b, c, d
        sr, si, tr, ti = ar + cr, ai + ci, ar - cr, ai - ci
        ur, ui, vr, vi = br + dr, bi + di, br - dr, bi - di
        if sign < 0:
            wr, wi = vi, -vr
            return (sr + ur, si + ui), (tr + vi, ti - vr), (sr - ur, si - ui), (tr - vi, ti + vr)
        return (sr + ur, si + ui), (tr - vi, ti + vr), (sr - ur, si - ui), (tr + vi, ti - vr)

    x = list(zip(re, im))
    mid = [four(x[n], x[n + 4], x[n + 8], x[n + 12]) for n in range(4)]
    out = [None] * 16
    h = np.float32(math.sqrt(0.5))
    for k1 in range(4):
        col = []
        for n2 in range(4):
            zr, zi = mid[n2][k1]
            m = n2 * k1
            if m == 0:
                pass
            elif m == 4:
                zr, zi = (zi, -zr) if sign < 0 else (-zi, zr)
            elif m == 2:
                zr, zi = ((zr + zi) * h, (zi - zr) * h) if sign < 0 else ((zr - zi) * h, (zi + zr) * h)
            elif m == 6:
                zr, zi = ((zi - zr) * h, -(zr + zi) * h) if sign < 0 else (-(zr + zi) * h, (zr - zi) * h)
            else:
                c = np.float32(math.cos(2 * math.pi * m / 16))
                s = np.float32(sign * math.sin(2 * math.pi * m / 16))
                zr, zi = zr * c - zi * s, zr * s + zi * c
            col.append((zr, zi))
        res = four(*col)
        for k2 in range(4):
            out[k1 + 4 * k2] = res[k2]
    return [o[0] for o in out], [o[1] for o in out]


def own_tiles(x_ref):
    return [swap_tile(x_ref[0, :, LANES * t:LANES * t + LANES].astype(F32)) for t in range(8)]


def place_centre(tiles, cen):
    for t in range(8):
        for pair in range(4):
            cen[pl.ds(t * 128 + pair, 32, stride=4), :] = tiles[t]


def spectral_kernel(kern_ref, ksp, kdp):
    tiles = [swap_tile(kern_ref[:, LANES * t:LANES * t + LANES]) for t in range(8)]
    whole = jnp.concatenate(tiles, axis=0)

    def exact(a, f):
        one = a.astype(BF16)
        rest = a - one.astype(F32)
        two = rest.astype(BF16)
        three = (rest - two.astype(F32)).astype(BF16)
        return f(one) + (f(two) + f(three))
    row = lax.broadcasted_iota(jnp.int32, (LANES, LANES), 0)
    col = lax.broadcasted_iota(jnp.int32, (LANES, LANES), 1)
    mirror = jnp.bitwise_and(-jnp.bitwise_and(col, 96), 96) + jnp.bitwise_and(-col, 31)
    perm = jnp.where(row == mirror, 1.0, 0.0).astype(BF16)
    row = lax.broadcasted_iota(jnp.int32, (32, 32), 0)
    col = lax.broadcasted_iota(jnp.int32, (32, 32), 1)
    flip = jnp.where(row == jnp.bitwise_and(-col, 31), 1.0, 0.0).astype(BF16)
    lanes = exact(whole, lambda v: jnp.dot(v, perm, preferred_element_type=F32))
    rev = [lanes[32 * t:32 * t + 32] for t in range(8)]
    wide = jnp.concatenate(rev, axis=1)
    wide = exact(wide, lambda v: jnp.dot(flip, v, preferred_element_type=F32))
    rev = [wide[:, LANES * t:LANES * t + LANES] for t in range(8)]
    lane = lax.broadcasted_iota(jnp.int32, (32, LANES), 1)
    sym = []
    for t in range(8):
        other = jnp.where(lane < 32, rev[(8 - t) % 8], rev[7 - t])
        sym.append((tiles[t] + other) * np.float32(0.5))

    def groups(parts):
        out = None
        for g, (t, j) in enumerate(parts):
            v = sym[t]
            if (g - j) % 4:
                v = pltpu.roll(v, 32 * ((g - j) % 4), 1)
            out = v if out is None else jnp.where(lane >= 32 * g, v, out)
        return out
    scale = np.float32(2.0 / 32768)
    u0 = groups([(0, 0), (1, 0), (2, 0), (3, 0)])
    edge = pltpu.roll(sym[4], 16, 1)
    u0 = jnp.where((lane >= 16) & (lane < 32), edge, u0)
    u0 = u0 * scale
    half = np.float32(1.0 / 65536)
    first = sym[0]
    second = pltpu.roll(sym[0], LANES - 16, 1)
    third = sym[4]
    mean0, diff0 = (first + second) * half, (first - second) * half
    fourth = pltpu.roll(sym[4], LANES - 16, 1)
    mean1, diff1 = (third + fourth) * half, (third - fourth) * half
    mean1, diff1 = pltpu.roll(mean1, 16, 1), pltpu.roll(diff1, 16, 1)
    u0 = jnp.where(lane == 0, mean0, jnp.where(lane == 16, mean1, u0))
    d0 = jnp.where(lane == 0, diff0, jnp.where(lane == 16, diff1, jnp.zeros_like(diff0)))
    u1 = groups([(t, 2) for t in range(4)]) * scale
    u2 = groups([(t, 1) for t in range(4)]) * scale
    u3 = groups([(t + 4, 1) for t in range(4)]) * scale
    for pair in range(4):
        for u, v in enumerate((u0, u1, u2, u3)):
            ksp[pl.ds(u * 128 + pair, 16, stride=8), :] = v[:16]
            ksp[pl.ds(u * 128 + 4 + pair, 16, stride=8), :] = v[16:]
        kdp[pl.ds(pair, 16, stride=8), :] = d0[:16]
        kdp[pl.ds(4 + pair, 16, stride=8), :] = d0[16:]


def shift_boxes(pool, tab, zero_plane, half_planes, m):
    lane = lax.broadcasted_iota(jnp.int32, (8, LANES), 1)
    sub = lax.broadcasted_iota(jnp.int32, (8, LANES), 0)
    a_id = jnp.bitwise_and(lane, 31)
    b_id = sub * 4 + lax.shift_right_logical(lane, 5)

    def one(k, _):
        base, oc, ob, oa, use = tab(k)
        s = ob * 32 + oa
        r = jnp.bitwise_and(s, 127)
        sh = jnp.bitwise_and(lax.shift_right_arithmetic(s, 7), 7)
        lane_by = jnp.bitwise_and(128 - r, 127)
        sub_by = jnp.bitwise_and(8 - sh, 7)
        keep = (a_id + oa >= 0) & (a_id + oa < 32) & (b_id + ob >= 0) & (b_id + ob < 32)
        near = lane < 128 - r
        row = (k // 4) * 128 + k % 4
        odd = jnp.bitwise_and(oc, 1)
        for par in range(2):
            first = base + jnp.where(odd == par, 0, 1) * half_planes
            off = jnp.where(use, lax.shift_right_arithmetic(oc + par, 1), 64)
            for n in range(16):
                at = n + off
                good = (at >= 0) & (at < 16)
                v = pool[jnp.where(good, first + at, zero_plane)].astype(F32)
                v = pltpu.roll(v, lane_by, 1)
                v = pltpu.roll(v, sub_by, 0)
                w = pltpu.roll(v, 7, 0)
                v = jnp.where(keep, jnp.where(near, v, w), 0.0)
                m[pl.ds(row + 4 * (2 * n + par), 8, stride=MST), :] = v
        return 0
    lax.fori_loop(0, PAIRS, one, 0)


def densities(m, cen, yh, yl):
    def one(i, _):
        row = pl.multiple_of(i * 16, 16)
        crow = pl.multiple_of(jnp.bitwise_and(i, 7) * 16, 16)
        x = [m[pl.ds(pl.multiple_of(MST * t + row, 8), 16), :]
             * cen[pl.ds(pl.multiple_of(128 * t + crow, 16), 16), :] for t in range(8)]
        for h in range(2):
            e, o = x[h] + x[4 + h], x[2 + h] + x[6 + h]
            d, g = x[h] - x[4 + h], x[6 + h] - x[2 + h]
            for at, v in ((0, e + o), (256, e - o), (512, d), (768, g)):
                hi, lo = split(v)
                yh[pl.ds(row, 16), at + LANES * h:at + LANES * h + LANES] = hi
                yl[pl.ds(row, 16), at + LANES * h:at + LANES * h + LANES] = lo
        return 0
    lax.fori_loop(0, 24, one, 0)


CUTS = ((0, 256), (256, 512), (512, 1024))


def turn(yh, yl, w, s, back):
    for (b, e), (wh, wl) in zip(CUTS, w):
        hi, lo = yh[:, b:e], yl[:, b:e]
        dims = (((1,), (1 if back else 0,)), ((), ()))

        def dot(p, q):
            return lax.dot_general(p, q, dims, preferred_element_type=F32)
        out = dot(hi, wh[...]) + dot(lo, wh[...]) + dot(hi, wl[...])
        for t in range(b // LANES, e // LANES):
            s[t] = out[:, t * LANES - b:t * LANES - b + LANES]


def filtered(s, yh, yl, ksp, kdp):
    sub = lax.broadcasted_iota(jnp.int32, (8, LANES), 0)
    lower = sub < 4
    sgn = jnp.where(lower, np.float32(1), np.float32(-1))

    def twiddle(k):
        c = np.float32(math.cos(2 * math.pi * k / 32))
        n = np.float32(math.sin(2 * math.pi * k / 32))
        return jnp.where(lower, np.float32(1), c), jnp.where(lower, np.float32(0), n)

    def job(g, tr, ti, krow, special, energy):
        row = pl.multiple_of(g * 128, 128)
        re = [s[tr, pl.ds(row + 8 * n, 8), :] for n in range(16)]
        im = [s[ti, pl.ds(row + 8 * n, 8), :] for n in range(16)]
        re, im = fft16(re, im, -1)
        zr, zi = [], []
        for k in range(16):
            r, i = re[k], im[k]
            if k:
                c, n = twiddle(k)
                r, i = r * c + i * n, i * c - r * n
            zr.append(pltpu.roll(r, 4, 0) + sgn * r)
            zi.append(pltpu.roll(i, 4, 0) + sgn * i)
        wr, wi = [], []
        for k in range(16):
            km = ksp[pl.ds(krow + 8 * k, 8), :]
            r, i = zr[k] * km, zi[k] * km
            if special:
                kd = kdp[pl.ds(8 * k, 8), :]
                fr, fi = zr[(16 - k) % 16], zi[(16 - k) % 16]
                if k:
                    fr, fi = pltpu.roll(fr, 4, 0), pltpu.roll(fi, 4, 0)
                r, i = r + kd * fr, i - kd * fi
            energy = energy + (r * zr[k] + i * zi[k])
            wr.append(r)
            wi.append(i)
        re, im = [], []
        for k in range(16):
            r = pltpu.roll(wr[k], 4, 0) + sgn * wr[k]
            i = pltpu.roll(wi[k], 4, 0) + sgn * wi[k]
            if k:
                c, n = twiddle(k)
                r, i = r * c - i * n, i * c + r * n
            re.append(r)
            im.append(i)
        re, im = fft16(re, im, 1)
        for n in range(0, 16, 2):
            for t, z in ((tr, re), (ti, im)):
                hi, lo = split(jnp.concatenate([z[n], z[n + 1]], axis=0))
                at = pl.ds(row + 8 * n, 16)
                lanes = pl.ds(pl.multiple_of(t * LANES, LANES), LANES)
                yh[at, lanes] = hi
                yl[at, lanes] = lo
        return energy

    energy = jnp.zeros((8, LANES), F32)

    def first(g, e):
        return job(g, 0, 1, 0, True, e)

    def other(i, e):
        g, u = i // 3, i % 3 + 1
        tr = jnp.where(u == 1, 2, u + 2)
        ti = jnp.where(u == 1, 3, u + 4)
        return job(g, tr, ti, pl.multiple_of(u * 128, 128), False, e)
    energy = lax.fori_loop(0, GROUPS, first, energy)
    return lax.fori_loop(0, 3 * GROUPS, other, energy)


def collect(s, m, acc):
    def one(i, _):
        row = pl.multiple_of(i * 8, 8)
        for h in range(2):
            total = [None] * 4
            for g in range(GROUPS):
                y0, y2, yr, yi = (s[2 * n + h, pl.ds(g * 128 + row, 8), :] for n in range(4))
                p, q = y0 + y2, y0 - y2
                for n, v in enumerate((p + yr, q - yi, p - yr, q + yi)):
                    v = v * m[pl.ds(MST * (2 * n + h) + g * 128 + row, 8), :]
                    total[n] = v if total[n] is None else total[n] + v
            for n in range(4):
                acc[pl.ds((2 * n + h) * 128 + row, 8), :] = total[n]
        return 0
    lax.fori_loop(0, 16, one, 0)


def summed_tiles(acc):
    out = []
    for t in range(8):
        v = [acc[pl.ds(t * 128 + pair, 32, stride=4), :] for pair in range(4)]
        out.append((v[0] + v[1]) + (v[2] + v[3]))
    return out


HALO = 3
KEEP = (
    {0: (0, 16), 1: (0, 16), 2: (0, 10), 3: (0, 4), -1: (1, 15), -2: (7, 9), -3: (13, 3)},
    {0: (0, 16), 1: (0, 15), 2: (0, 9), 3: (0, 3), -1: (0, 16), -2: (6, 10), -3: (12, 4)},
)
MESH = pl.DeviceIdType.MESH


def sign(v):
    return (v > 0) - (v < 0)


ORB_HOP = {1: 1, 2: 2, 3: 3, 4: 4}
SLAB_HOP = {1: 1, 2: 2, 3: 3}
LATE_HOP = {1: 1, 2: 1, 3: 1, 4: 1}


def routes(n_orb):
    out = []
    for core in range(2):
        tree = {}
        for dz in range(-HALO, HALO + 1):
            for dx in range(1 - n_orb // 2, n_orb // 2 + 1):
                if (dz, dx) == (0, 0):
                    continue
                way = sign(dx)
                if dx == n_orb // 2 and core == 1 and dz in (0, -1, -2):
                    way = -1
                if core == 0:
                    tree[dz, dx] = (sign(dz) * SLAB_HOP[abs(dz)], 0) if dz else (0, way * ORB_HOP[abs(dx)])
                else:
                    tree[dz, dx] = (0, way * LATE_HOP[abs(dx)]) if dx else (sign(dz) * SLAB_HOP[abs(dz)], 0)
        out.append(tree)
    return out


def held_as(tree, p, n_orb):
    dz, dx = p[0] - tree[p][0], p[1] - tree[p][1]
    return dz, (dx + n_orb // 2 - 1) % n_orb - n_orb // 2 + 1


def schedule(tree, n_orb):
    def depth(p):
        return 0 if p == (0, 0) else 1 + depth(held_as(tree, p, n_orb))
    return sorted(tree, key=lambda p: (depth(p), abs(p[0]) + abs(p[1]), p))


def kernel_body(n_slab, n_orb, x_hbm, corners_hbm, partners_hbm, kern_hbm, *rest):
    w_hbm, rest = rest[:2], rest[2:]
    out_ref, en_ref = rest[:2]
    (pool, m, yh, yl, s, ksp, kdp, cen, acc, kern, part, other, ex, ez) = rest[2:16]
    w_ref = rest[16:18]
    x_ref, corners, partners = rest[18:21]
    local_sem, send_sem, recv_sem, swap_send, swap_recv, tail_sem, ready_one, ready_two = rest[21:]
    here_x = lax.axis_index("orb")
    here_z = lax.axis_index("slab")
    rep = lax.axis_index("rep")
    blocks = (2 * HALO + 1) * n_orb
    zero_plane = 2 * blocks * 16

    def at_slab(step):
        return {"slab": lax.rem(here_z + step + n_slab, n_slab)}

    def at_orb(step):
        return {"orb": lax.rem(here_x + step + n_orb, n_orb)}
    sibling = {"rep": 1 - rep}

    trees = routes(n_orb)

    def at(hop):
        return {**at_slab(hop[0]), **at_orb(hop[1])}
    barrier = pltpu.get_barrier_semaphore()
    pl.semaphore_signal(barrier, inc=1, device_id=sibling, device_id_type=MESH)
    for core in range(2):
        @pl.when(rep == core)
        def _(core=core):
            for hop in sorted(set(trees[core].values())):
                pl.semaphore_signal(barrier, inc=1, device_id=at(hop), device_id_type=MESH)

    x_load = pltpu.make_async_copy(x_hbm, x_ref, local_sem.at[0])
    x_load.start()
    loads = [pltpu.make_async_copy(a, b, local_sem.at[1 + i]) for i, (a, b) in enumerate(zip(
        (kern_hbm, corners_hbm, partners_hbm) + w_hbm, (kern, corners, partners) + w_ref))]
    for load in loads:
        load.start()
    x_load.wait()
    tiles = own_tiles(x_ref)
    for t in range(8):
        acc[pl.ds(t, 32, stride=8), :] = tiles[t]
    own_block = HALO * n_orb + here_x
    mine = rep * blocks + own_block
    for c in range(16):
        even = acc[16 * c:16 * c + 8, :]
        odd = acc[16 * c + 8:16 * c + 16, :]
        pool[mine * 16 + c] = jnp.where(rep == 0, even, odd).astype(BF16)
    pool[zero_plane] = jnp.zeros((8, LANES), BF16)
    for core in range(2):
        @pl.when(rep == core)
        def _(core=core):
            pl.semaphore_wait(barrier, len(set(trees[core].values())) + 1)

    def signal_far(sem):
        for step in (HALO, -HALO):
            pl.semaphore_signal(sem, inc=1, device_id=at_slab(step), device_id_type=MESH)

    def slot(core, p):
        first, count = KEEP[core][p[0]]
        block = core * blocks + (p[0] + HALO) * n_orb + lax.rem(here_x + p[1] + n_orb, n_orb)
        return pool.at[pl.ds(block * 16 + first, count)]

    def index(p):
        return (p[0] + HALO) * n_orb + (p[1] + n_orb) % n_orb

    def swap(core, p):
        return pltpu.make_async_remote_copy(
            src_ref=slot(core, p), dst_ref=slot(core, p), send_sem=swap_send.at[index(p)],
            recv_sem=swap_recv.at[index(p)], device_id=sibling, device_id_type=MESH)

    def pass_on(core, p, hop):
        first, count = KEEP[core][p[0]]
        held = (p[0] - hop[0], p[1] - hop[1])
        x_slot = lax.rem(here_x + held[1] + n_orb, n_orb)
        src = pool.at[pl.ds((core * blocks + (held[0] + HALO) * n_orb + x_slot) * 16 + first, count)]
        dst = pool.at[pl.ds((core * blocks + (p[0] + HALO) * n_orb + x_slot) * 16 + first, count)]
        peer = at((-hop[0], -hop[1]))
        return pltpu.make_async_remote_copy(
            src_ref=src, dst_ref=dst, send_sem=send_sem.at[index(p)], recv_sem=recv_sem.at[index(p)],
            device_id=peer, device_id_type=MESH)

    def arrival(core, p):
        return pltpu.make_async_remote_copy(
            src_ref=slot(core, p), dst_ref=slot(core, p), send_sem=send_sem.at[index(p)],
            recv_sem=recv_sem.at[index(p)], device_id=sibling, device_id_type=MESH)

    def spread(core, held):
        tree = trees[core]
        for p in sorted(tree, key=lambda p: -abs(tree[p][0]) - abs(tree[p][1])):
            if held_as(tree, p, n_orb) == held:
                pass_on(core, p, tree[p]).start()
        swap(core, held).start()

    for core in range(2):
        @pl.when(rep == core)
        def _(core=core):
            spread(core, (0, 0))

    signal_far(ready_one)
    place_centre(tiles, cen)
    loads[0].wait()
    spectral_kernel(kern, ksp, kdp)

    for core in range(2):
        @pl.when(rep == core)
        def _(core=core):
            for p in schedule(trees[core], n_orb):
                arrival(core, p).wait_recv()
                spread(core, p)
            for p in trees[core]:
                arrival(core, p).wait_send()
            for p in [(0, 0)] + list(trees[core]):
                swap(core, p).wait_send()
                swap(1 - core, p).wait_recv()

    pl.semaphore_wait(ready_one, 2)
    signal_far(ready_two)

    own = here_z * n_orb + here_x

    def wrap(v):
        v = v + G // 2
        v = jnp.where(v < 0, v + G, jnp.where(v >= G, v - G, v))
        return v - G // 2

    loads[1].wait()
    loads[2].wait()

    def tab(k):
        j = partners[0, 2 * k + rep]
        use = j >= 0
        j = jnp.where(use, j, own)
        o = [wrap(corners[d, own] - corners[d, j]) for d in range(3)]
        dz = lax.div(j, n_orb) - here_z
        dz = jnp.where(dz > n_slab // 2, dz - n_slab, jnp.where(dz < -(n_slab // 2), dz + n_slab, dz))
        dz = jnp.clip(dz, -HALO, HALO)
        return ((dz + HALO) * n_orb + lax.rem(j, n_orb)) * 16, o[2], o[1], o[0], use

    shift_boxes(pool, tab, zero_plane, blocks * 16, m)
    densities(m, cen, yh, yl)
    for load in loads[3:]:
        load.wait()
    w = [(w_ref[0].at[pl.ds(a, 256)], w_ref[0].at[pl.ds(a + 256, 256)]) for a in (0, 512)]
    w.append((w_ref[1].at[pl.ds(0, 512)], w_ref[1].at[pl.ds(512, 512)]))
    turn(yh, yl, w, s, False)
    energy = filtered(s, yh, yl, ksp, kdp)
    pl.semaphore_wait(ready_two, 2)

    me = 2 * here_x + rep
    ex[me] = jnp.sum(energy, axis=0, keepdims=True)

    def to_slab(step, cross, back):
        other_rep = 1 - rep if cross else rep
        there = 2 * lax.rem(here_x - step + n_orb, n_orb) + other_rep
        cell = ex.at[there if back else me]
        n = 2 * step + cross
        return pltpu.make_async_remote_copy(
            src_ref=cell, dst_ref=cell, send_sem=tail_sem.at[2 + n], recv_sem=tail_sem.at[2 + 2 * n_orb + n],
            device_id={**at_orb(step), "rep": other_rep}, device_id_type=MESH)

    def to_column(step, back):
        cell = ez.at[lax.rem(here_z - step + n_slab, n_slab) if back else here_z]
        first = 2 + 4 * n_orb
        return pltpu.make_async_remote_copy(
            src_ref=cell, dst_ref=cell, send_sem=tail_sem.at[first + step],
            recv_sem=tail_sem.at[first + n_slab + step], device_id=at_slab(step), device_id_type=MESH)
    near = [(step, cross) for step in range(n_orb) for cross in range(2) if step or cross]
    near.sort(key=lambda v: -min(v[0], n_orb - v[0]))
    far = sorted(range(1, n_slab), key=lambda v: -min(v, n_slab - v))
    for step, cross in near:
        to_slab(step, cross, False).start()
    turn(yh, yl, w, s, True)
    collect(s, m, acc)
    res = summed_tiles(acc)
    for t in range(8):
        part[t] = res[t]
    swap_part = pltpu.make_async_remote_copy(
        src_ref=part, dst_ref=other, send_sem=tail_sem.at[0], recv_sem=tail_sem.at[1],
        device_id=sibling, device_id_type=MESH)
    swap_part.start()
    for step, cross in near:
        to_slab(step, cross, True).wait_recv()
    ez[here_z] = functools.reduce(lambda a, b: a + b, [ex[i] for i in range(2 * n_orb)])
    for step in far:
        to_column(step, False).start()
    swap_part.wait()
    for t in range(8):
        kern[:, LANES * t:LANES * t + LANES] = -swap_tile(part[t] + other[t])
    flush = pltpu.make_async_copy(kern, out_ref.at[0], local_sem.at[0])
    flush.start()
    for step, cross in near:
        to_slab(step, cross, False).wait_send()
    for step in far:
        to_column(step, True).wait_recv()
    total = functools.reduce(lambda a, b: a + b, [ez[i] for i in range(n_slab)])
    for step in far:
        to_column(step, False).wait_send()
    flush.wait()
    en_ref[0] = jnp.sum(total) * np.float32(-1.0 / (2.0 * n_slab * n_orb * B ** 3))


def body(n_slab, n_orb, orbitals, corners, partners, kernel):
    blocks = (2 * HALO + 1) * n_orb
    smem = pl.BlockSpec(memory_space=pltpu.SMEM)
    hbm = pl.BlockSpec(memory_space=pl.ANY)
    dma = pltpu.SemaphoreType.DMA
    tables = plane_tables()
    weights = [jnp.asarray(np.concatenate(tables[:4])), jnp.asarray(np.concatenate(tables[4:]))]
    return pl.pallas_call(
        functools.partial(kernel_body, n_slab, n_orb),
        out_shape=(jax.ShapeDtypeStruct((1, B, B * B), F32), jax.ShapeDtypeStruct((1,), F32)),
        in_specs=[hbm] * 6,
        out_specs=(hbm, smem),
        scratch_shapes=[
            pltpu.VMEM((2 * blocks * 16 + 1, 8, LANES), BF16),
            pltpu.VMEM((8 * MST, LANES), F32),
            pltpu.VMEM((384, 1024), BF16),
            pltpu.VMEM((384, 1024), BF16),
            pltpu.VMEM((8, 384, LANES), F32),
            pltpu.VMEM((512, LANES), F32),
            pltpu.VMEM((128, LANES), F32),
            pltpu.VMEM((1024, LANES), F32),
            pltpu.VMEM((1024, LANES), F32),
            pltpu.VMEM((B, B * B), F32),
            pltpu.VMEM((8, B, LANES), F32),
            pltpu.VMEM((8, B, LANES), F32),
            pltpu.VMEM((2 * n_orb, 1, LANES), F32),
            pltpu.VMEM((n_slab, 1, LANES), F32),
            *[pltpu.VMEM(w.shape, BF16) for w in weights],
            pltpu.VMEM((1, B, B * B), BF16),
            pltpu.SMEM(corners.shape[::-1], jnp.int32),
            pltpu.SMEM(partners.shape, jnp.int32),
            dma((6,)),
            dma((blocks,)),
            dma((blocks,)),
            dma((blocks,)),
            dma((blocks,)),
            dma((2 + 4 * n_orb + 2 * n_slab,)),
            pltpu.SemaphoreType.REGULAR,
            pltpu.SemaphoreType.REGULAR,
        ],
        compiler_params=pltpu.CompilerParams(
            collective_id=0, has_side_effects=True, vmem_limit_bytes=67043328),
    )(orbitals, corners.T, partners, kernel, *weights)


def solution(mesh):
    in_specs = (
        P(("grp", "slab", "orb"), None, None),
        P("grp", None),
        P(("grp", "slab", "orb"), None),
        P(),
    )
    out_specs = (P(("grp", "slab", "orb"), None, None), P("grp"))
    step = functools.partial(body, mesh.shape["slab"], mesh.shape["orb"])
    return jax.shard_map(step, mesh=mesh, in_specs=in_specs, out_specs=out_specs, check_vma=False)
```

```python
import functools, math
import jax, jax.numpy as jnp, numpy as np
from jax import lax
from jax.experimental import pallas as pl
from jax.sharding import PartitionSpec as P
from jax.experimental.pallas import tpu as pltpu

G = 192
ZDEV = 12
B = 32
LANES = 128
PAIRS = 12
GROUPS = 3
MST = 392
F32 = jnp.float32
BF16 = jnp.bfloat16


def plane_tables():
    def th(q, p, bl, a):
        return 2 * np.pi * ((q * bl + p * a) % 32) / 32
    bl = np.repeat(np.arange(8), 32)[:, None]
    a = np.tile(np.arange(32), 8)[:, None]
    lane = np.arange(128)
    g, r = lane // 32, lane % 32
    q = np.where(g > 0, 4 * g, np.where(r < 16, 0, 16))
    p = np.where(g > 0, r, r % 16)
    t = th(q, p, bl, a)
    w0 = np.concatenate([np.cos(t), -np.sin(t)], 1)
    for l in (0, 16):
        w0[:, 128 + l] = np.cos(th(q[l], 16, bl, a))[:, 0]
    t = th(2 + 4 * g, r, bl, a)
    w2 = np.concatenate([np.cos(t), -np.sin(t)], 1)
    l2 = np.arange(256)
    t = th(1 + 4 * (l2 // 32), l2 % 32, bl, a)
    c, s = np.cos(t), np.sin(t)
    w1 = np.block([[c, -s], [s, c]])
    out = []
    for w in (w0, w2, w1):
        w = w.astype(np.float32)
        hi = w.astype(jnp.bfloat16)
        lo = (w - hi.astype(np.float32)).astype(jnp.bfloat16)
        out += [hi, lo]
    return out


def split(x):
    hi = x.astype(BF16)
    return hi, (x - hi.astype(F32)).astype(BF16)


def swap_tile(x):
    t = x.T
    return jnp.concatenate([t[32 * j:32 * j + 32] for j in range(4)], axis=1)


def fft16(re, im, sign):
    def four(a, b, c, d):
        (ar, ai), (br, bi), (cr, ci), (dr, di) = a, b, c, d
        sr, si, tr, ti = ar + cr, ai + ci, ar - cr, ai - ci
        ur, ui, vr, vi = br + dr, bi + di, br - dr, bi - di
        if sign < 0:
            wr, wi = vi, -vr
            return (sr + ur, si + ui), (tr + vi, ti - vr), (sr - ur, si - ui), (tr - vi, ti + vr)
        return (sr + ur, si + ui), (tr - vi, ti + vr), (sr - ur, si - ui), (tr + vi, ti - vr)

    x = list(zip(re, im))
    mid = [four(x[n], x[n + 4], x[n + 8], x[n + 12]) for n in range(4)]
    out = [None] * 16
    h = np.float32(math.sqrt(0.5))
    for k1 in range(4):
        col = []
        for n2 in range(4):
            zr, zi = mid[n2][k1]
            m = n2 * k1
            if m == 0:
                pass
            elif m == 4:
                zr, zi = (zi, -zr) if sign < 0 else (-zi, zr)
            elif m == 2:
                zr, zi = ((zr + zi) * h, (zi - zr) * h) if sign < 0 else ((zr - zi) * h, (zi + zr) * h)
            elif m == 6:
                zr, zi = ((zi - zr) * h, -(zr + zi) * h) if sign < 0 else (-(zr + zi) * h, (zr - zi) * h)
            else:
                c = np.float32(math.cos(2 * math.pi * m / 16))
                s = np.float32(sign * math.sin(2 * math.pi * m / 16))
                zr, zi = zr * c - zi * s, zr * s + zi * c
            col.append((zr, zi))
        res = four(*col)
        for k2 in range(4):
            out[k1 + 4 * k2] = res[k2]
    return [o[0] for o in out], [o[1] for o in out]


def own_tiles(x_ref):
    return [swap_tile(x_ref[0, :, LANES * t:LANES * t + LANES].astype(F32)) for t in range(8)]


def place_centre(tiles, cen):
    for t in range(8):
        for pair in range(4):
            cen[pl.ds(t * 128 + pair, 32, stride=4), :] = tiles[t]


def spectral_kernel(kern_ref, ksp, kdp):
    tiles = [swap_tile(kern_ref[:, LANES * t:LANES * t + LANES]) for t in range(8)]
    whole = jnp.concatenate(tiles, axis=0)

    def exact(a, f):
        one = a.astype(BF16)
        rest = a - one.astype(F32)
        two = rest.astype(BF16)
        three = (rest - two.astype(F32)).astype(BF16)
        return f(one) + (f(two) + f(three))
    row = lax.broadcasted_iota(jnp.int32, (LANES, LANES), 0)
    col = lax.broadcasted_iota(jnp.int32, (LANES, LANES), 1)
    mirror = jnp.bitwise_and(-jnp.bitwise_and(col, 96), 96) + jnp.bitwise_and(-col, 31)
    perm = jnp.where(row == mirror, 1.0, 0.0).astype(BF16)
    row = lax.broadcasted_iota(jnp.int32, (32, 32), 0)
    col = lax.broadcasted_iota(jnp.int32, (32, 32), 1)
    flip = jnp.where(row == jnp.bitwise_and(-col, 31), 1.0, 0.0).astype(BF16)
    lanes = exact(whole, lambda v: jnp.dot(v, perm, preferred_element_type=F32))
    rev = [lanes[32 * t:32 * t + 32] for t in range(8)]
    wide = jnp.concatenate(rev, axis=1)
    wide = exact(wide, lambda v: jnp.dot(flip, v, preferred_element_type=F32))
    rev = [wide[:, LANES * t:LANES * t + LANES] for t in range(8)]
    lane = lax.broadcasted_iota(jnp.int32, (32, LANES), 1)
    sym = []
    for t in range(8):
        other = jnp.where(lane < 32, rev[(8 - t) % 8], rev[7 - t])
        sym.append((tiles[t] + other) * np.float32(0.5))

    def groups(parts):
        out = None
        for g, (t, j) in enumerate(parts):
            v = sym[t]
            if (g - j) % 4:
                v = pltpu.roll(v, 32 * ((g - j) % 4), 1)
            out = v if out is None else jnp.where(lane >= 32 * g, v, out)
        return out
    scale = np.float32(2.0 / 32768)
    u0 = groups([(0, 0), (1, 0), (2, 0), (3, 0)])
    edge = pltpu.roll(sym[4], 16, 1)
    u0 = jnp.where((lane >= 16) & (lane < 32), edge, u0)
    u0 = u0 * scale
    half = np.float32(1.0 / 65536)
    first = sym[0]
    second = pltpu.roll(sym[0], LANES - 16, 1)
    third = sym[4]
    mean0, diff0 = (first + second) * half, (first - second) * half
    fourth = pltpu.roll(sym[4], LANES - 16, 1)
    mean1, diff1 = (third + fourth) * half, (third - fourth) * half
    mean1, diff1 = pltpu.roll(mean1, 16, 1), pltpu.roll(diff1, 16, 1)
    u0 = jnp.where(lane == 0, mean0, jnp.where(lane == 16, mean1, u0))
    d0 = jnp.where(lane == 0, diff0, jnp.where(lane == 16, diff1, jnp.zeros_like(diff0)))
    u1 = groups([(t, 2) for t in range(4)]) * scale
    u2 = groups([(t, 1) for t in range(4)]) * scale
    u3 = groups([(t + 4, 1) for t in range(4)]) * scale
    for pair in range(4):
        for u, v in enumerate((u0, u1, u2, u3)):
            ksp[pl.ds(u * 128 + pair, 16, stride=8), :] = v[:16]
            ksp[pl.ds(u * 128 + 4 + pair, 16, stride=8), :] = v[16:]
        kdp[pl.ds(pair, 16, stride=8), :] = d0[:16]
        kdp[pl.ds(4 + pair, 16, stride=8), :] = d0[16:]


def shift_boxes(pool, tab, zero_plane, half_planes, m):
    lane = lax.broadcasted_iota(jnp.int32, (8, LANES), 1)
    sub = lax.broadcasted_iota(jnp.int32, (8, LANES), 0)
    a_id = jnp.bitwise_and(lane, 31)
    b_id = sub * 4 + lax.shift_right_logical(lane, 5)

    def one(k, _):
        base, oc, ob, oa, use = tab(k)
        s = ob * 32 + oa
        r = jnp.bitwise_and(s, 127)
        sh = jnp.bitwise_and(lax.shift_right_arithmetic(s, 7), 7)
        lane_by = jnp.bitwise_and(128 - r, 127)
        sub_by = jnp.bitwise_and(8 - sh, 7)
        keep = (a_id + oa >= 0) & (a_id + oa < 32) & (b_id + ob >= 0) & (b_id + ob < 32)
        near = lane < 128 - r
        row = (k // 4) * 128 + k % 4
        odd = jnp.bitwise_and(oc, 1)
        for par in range(2):
            first = base + jnp.where(odd == par, 0, 1) * half_planes
            off = jnp.where(use, lax.shift_right_arithmetic(oc + par, 1), 64)
            for n in range(16):
                at = n + off
                good = (at >= 0) & (at < 16)
                v = pool[jnp.where(good, first + at, zero_plane)].astype(F32)
                v = pltpu.roll(v, lane_by, 1)
                v = pltpu.roll(v, sub_by, 0)
                w = pltpu.roll(v, 7, 0)
                v = jnp.where(keep, jnp.where(near, v, w), 0.0)
                m[pl.ds(row + 4 * (2 * n + par), 8, stride=MST), :] = v
        return 0
    lax.fori_loop(0, PAIRS, one, 0)


def densities(m, cen, yh, yl):
    def one(i, _):
        row = pl.multiple_of(i * 16, 16)
        crow = pl.multiple_of(jnp.bitwise_and(i, 7) * 16, 16)
        x = [m[pl.ds(pl.multiple_of(MST * t + row, 8), 16), :]
             * cen[pl.ds(pl.multiple_of(128 * t + crow, 16), 16), :] for t in range(8)]
        for h in range(2):
            e, o = x[h] + x[4 + h], x[2 + h] + x[6 + h]
            d, g = x[h] - x[4 + h], x[6 + h] - x[2 + h]
            for at, v in ((0, e + o), (256, e - o), (512, d), (768, g)):
                hi, lo = split(v)
                yh[pl.ds(row, 16), at + LANES * h:at + LANES * h + LANES] = hi
                yl[pl.ds(row, 16), at + LANES * h:at + LANES * h + LANES] = lo
        return 0
    lax.fori_loop(0, 24, one, 0)


CUTS = ((0, 256), (256, 512), (512, 1024))


def turn(yh, yl, w, s, back):
    for (b, e), (wh, wl) in zip(CUTS, w):
        hi, lo = yh[:, b:e], yl[:, b:e]
        dims = (((1,), (1 if back else 0,)), ((), ()))

        def dot(p, q):
            return lax.dot_general(p, q, dims, preferred_element_type=F32)
        out = dot(hi, wh[...]) + dot(lo, wh[...]) + dot(hi, wl[...])
        for t in range(b // LANES, e // LANES):
            s[t] = out[:, t * LANES - b:t * LANES - b + LANES]


def filtered(s, yh, yl, ksp, kdp):
    sub = lax.broadcasted_iota(jnp.int32, (8, LANES), 0)
    lower = sub < 4
    sgn = jnp.where(lower, np.float32(1), np.float32(-1))

    def twiddle(k):
        c = np.float32(math.cos(2 * math.pi * k / 32))
        n = np.float32(math.sin(2 * math.pi * k / 32))
        return jnp.where(lower, np.float32(1), c), jnp.where(lower, np.float32(0), n)

    def job(g, tr, ti, krow, special, energy):
        row = pl.multiple_of(g * 128, 128)
        re = [s[tr, pl.ds(row + 8 * n, 8), :] for n in range(16)]
        im = [s[ti, pl.ds(row + 8 * n, 8), :] for n in range(16)]
        re, im = fft16(re, im, -1)
        zr, zi = [], []
        for k in range(16):
            r, i = re[k], im[k]
            if k:
                c, n = twiddle(k)
                r, i = r * c + i * n, i * c - r * n
            zr.append(pltpu.roll(r, 4, 0) + sgn * r)
            zi.append(pltpu.roll(i, 4, 0) + sgn * i)
        wr, wi = [], []
        for k in range(16):
            km = ksp[pl.ds(krow + 8 * k, 8), :]
            r, i = zr[k] * km, zi[k] * km
            if special:
                kd = kdp[pl.ds(8 * k, 8), :]
                fr, fi = zr[(16 - k) % 16], zi[(16 - k) % 16]
                if k:
                    fr, fi = pltpu.roll(fr, 4, 0), pltpu.roll(fi, 4, 0)
                r, i = r + kd * fr, i - kd * fi
            energy = energy + (r * zr[k] + i * zi[k])
            wr.append(r)
            wi.append(i)
        re, im = [], []
        for k in range(16):
            r = pltpu.roll(wr[k], 4, 0) + sgn * wr[k]
            i = pltpu.roll(wi[k], 4, 0) + sgn * wi[k]
            if k:
                c, n = twiddle(k)
                r, i = r * c - i * n, i * c + r * n
            re.append(r)
            im.append(i)
        re, im = fft16(re, im, 1)
        for n in range(0, 16, 2):
            for t, z in ((tr, re), (ti, im)):
                hi, lo = split(jnp.concatenate([z[n], z[n + 1]], axis=0))
                at = pl.ds(row + 8 * n, 16)
                lanes = pl.ds(pl.multiple_of(t * LANES, LANES), LANES)
                yh[at, lanes] = hi
                yl[at, lanes] = lo
        return energy

    energy = jnp.zeros((8, LANES), F32)

    def first(g, e):
        return job(g, 0, 1, 0, True, e)

    def other(i, e):
        g, u = i // 3, i % 3 + 1
        tr = jnp.where(u == 1, 2, u + 2)
        ti = jnp.where(u == 1, 3, u + 4)
        return job(g, tr, ti, pl.multiple_of(u * 128, 128), False, e)
    energy = lax.fori_loop(0, GROUPS, first, energy)
    return lax.fori_loop(0, 3 * GROUPS, other, energy)


def collect(s, m, acc):
    def one(i, _):
        row = pl.multiple_of(i * 8, 8)
        for h in range(2):
            total = [None] * 4
            for g in range(GROUPS):
                y0, y2, yr, yi = (s[2 * n + h, pl.ds(g * 128 + row, 8), :] for n in range(4))
                p, q = y0 + y2, y0 - y2
                for n, v in enumerate((p + yr, q - yi, p - yr, q + yi)):
                    v = v * m[pl.ds(MST * (2 * n + h) + g * 128 + row, 8), :]
                    total[n] = v if total[n] is None else total[n] + v
            for n in range(4):
                acc[pl.ds((2 * n + h) * 128 + row, 8), :] = total[n]
        return 0
    lax.fori_loop(0, 16, one, 0)


def summed_tiles(acc):
    out = []
    for t in range(8):
        v = [acc[pl.ds(t * 128 + pair, 32, stride=4), :] for pair in range(4)]
        out.append((v[0] + v[1]) + (v[2] + v[3]))
    return out


HALO = 3
KEEP = (
    {0: (0, 16), 1: (0, 16), 2: (0, 10), 3: (0, 4), -1: (1, 15), -2: (7, 9), -3: (13, 3)},
    {0: (0, 16), 1: (0, 15), 2: (0, 9), 3: (0, 3), -1: (0, 16), -2: (6, 10), -3: (12, 4)},
)
MESH = pl.DeviceIdType.MESH


def sign(v):
    return (v > 0) - (v < 0)


ORB_HOP = {1: 1, 2: 2, 3: 3, 4: 4}
SLAB_HOP = {1: 1, 2: 2, 3: 3}
LATE_HOP = {1: 1, 2: 2, 3: 1, 4: 2}


def routes(n_orb):
    out = []
    for core in range(2):
        tree = {}
        for dz in range(-HALO, HALO + 1):
            for dx in range(1 - n_orb // 2, n_orb // 2 + 1):
                if (dz, dx) == (0, 0):
                    continue
                way = sign(dx)
                if dx == n_orb // 2 and core == 0 and dz in (0, -1, -2):
                    way = -1
                if core == 1:
                    tree[dz, dx] = (sign(dz) * SLAB_HOP[abs(dz)], 0) if dz else (0, way * ORB_HOP[abs(dx)])
                else:
                    tree[dz, dx] = (0, way * LATE_HOP[abs(dx)]) if dx else (sign(dz) * SLAB_HOP[abs(dz)], 0)
        out.append(tree)
    return out


def held_as(tree, p, n_orb):
    dz, dx = p[0] - tree[p][0], p[1] - tree[p][1]
    return dz, (dx + n_orb // 2 - 1) % n_orb - n_orb // 2 + 1


def schedule(tree, n_orb):
    def depth(p):
        return 0 if p == (0, 0) else 1 + depth(held_as(tree, p, n_orb))
    return sorted(tree, key=lambda p: (depth(p), abs(p[0]) + abs(p[1]), p))


def kernel_body(n_slab, n_orb, x_hbm, corners_hbm, partners_hbm, kern_hbm, *rest):
    w_hbm, rest = rest[:2], rest[2:]
    out_ref, en_ref = rest[:2]
    (pool, m, yh, yl, s, ksp, kdp, cen, acc, kern, part, other, ex, ez) = rest[2:16]
    w_ref = rest[16:18]
    x_ref, corners, partners = rest[18:21]
    local_sem, send_sem, recv_sem, swap_send, swap_recv, tail_sem, ready_one, ready_two = rest[21:]
    here_x = lax.axis_index("orb")
    here_z = lax.axis_index("slab")
    rep = lax.axis_index("rep")
    blocks = (2 * HALO + 1) * n_orb
    zero_plane = 2 * blocks * 16

    def at_slab(step):
        return {"slab": lax.rem(here_z + step + n_slab, n_slab)}

    def at_orb(step):
        return {"orb": lax.rem(here_x + step + n_orb, n_orb)}
    sibling = {"rep": 1 - rep}

    trees = routes(n_orb)

    def at(hop):
        return {**at_slab(hop[0]), **at_orb(hop[1])}
    barrier = pltpu.get_barrier_semaphore()
    pl.semaphore_signal(barrier, inc=1, device_id=sibling, device_id_type=MESH)
    for core in range(2):
        @pl.when(rep == core)
        def _(core=core):
            for hop in sorted(set(trees[core].values())):
                pl.semaphore_signal(barrier, inc=1, device_id=at(hop), device_id_type=MESH)

    x_load = pltpu.make_async_copy(x_hbm, x_ref, local_sem.at[0])
    x_load.start()
    loads = [pltpu.make_async_copy(a, b, local_sem.at[1 + i]) for i, (a, b) in enumerate(zip(
        (kern_hbm, corners_hbm, partners_hbm) + w_hbm, (kern, corners, partners) + w_ref))]
    for load in loads:
        load.start()
    x_load.wait()
    tiles = own_tiles(x_ref)
    for t in range(8):
        acc[pl.ds(t, 32, stride=8), :] = tiles[t]
    own_block = HALO * n_orb + here_x
    mine = rep * blocks + own_block
    for c in range(16):
        even = acc[16 * c:16 * c + 8, :]
        odd = acc[16 * c + 8:16 * c + 16, :]
        pool[mine * 16 + c] = jnp.where(rep == 0, even, odd).astype(BF16)
    pool[zero_plane] = jnp.zeros((8, LANES), BF16)
    for core in range(2):
        @pl.when(rep == core)
        def _(core=core):
            pl.semaphore_wait(barrier, len(set(trees[core].values())) + 1)

    def signal_far(sem):
        for step in (HALO, -HALO):
            pl.semaphore_signal(sem, inc=1, device_id=at_slab(step), device_id_type=MESH)

    def slot(core, p):
        first, count = KEEP[core][p[0]]
        block = core * blocks + (p[0] + HALO) * n_orb + lax.rem(here_x + p[1] + n_orb, n_orb)
        return pool.at[pl.ds(block * 16 + first, count)]

    def index(p):
        return (p[0] + HALO) * n_orb + (p[1] + n_orb) % n_orb

    def swap(core, p):
        return pltpu.make_async_remote_copy(
            src_ref=slot(core, p), dst_ref=slot(core, p), send_sem=swap_send.at[index(p)],
            recv_sem=swap_recv.at[index(p)], device_id=sibling, device_id_type=MESH)

    def pass_on(core, p, hop):
        first, count = KEEP[core][p[0]]
        held = (p[0] - hop[0], p[1] - hop[1])
        x_slot = lax.rem(here_x + held[1] + n_orb, n_orb)
        src = pool.at[pl.ds((core * blocks + (held[0] + HALO) * n_orb + x_slot) * 16 + first, count)]
        dst = pool.at[pl.ds((core * blocks + (p[0] + HALO) * n_orb + x_slot) * 16 + first, count)]
        peer = at((-hop[0], -hop[1]))
        return pltpu.make_async_remote_copy(
            src_ref=src, dst_ref=dst, send_sem=send_sem.at[index(p)], recv_sem=recv_sem.at[index(p)],
            device_id=peer, device_id_type=MESH)

    def arrival(core, p):
        return pltpu.make_async_remote_copy(
            src_ref=slot(core, p), dst_ref=slot(core, p), send_sem=send_sem.at[index(p)],
            recv_sem=recv_sem.at[index(p)], device_id=sibling, device_id_type=MESH)

    def spread(core, held):
        tree = trees[core]
        for p in sorted(tree, key=lambda p: abs(tree[p][0]) + abs(tree[p][1])):
            if held_as(tree, p, n_orb) == held:
                pass_on(core, p, tree[p]).start()
        swap(core, held).start()

    for core in range(2):
        @pl.when(rep == core)
        def _(core=core):
            spread(core, (0, 0))

    signal_far(ready_one)
    place_centre(tiles, cen)
    loads[0].wait()
    spectral_kernel(kern, ksp, kdp)

    for core in range(2):
        @pl.when(rep == core)
        def _(core=core):
            for p in schedule(trees[core], n_orb):
                arrival(core, p).wait_recv()
                spread(core, p)
            for p in trees[core]:
                arrival(core, p).wait_send()
            for p in [(0, 0)] + list(trees[core]):
                swap(core, p).wait_send()
                swap(1 - core, p).wait_recv()

    pl.semaphore_wait(ready_one, 2)
    signal_far(ready_two)

    own = here_z * n_orb + here_x

    def wrap(v):
        v = v + G // 2
        v = jnp.where(v < 0, v + G, jnp.where(v >= G, v - G, v))
        return v - G // 2

    loads[1].wait()
    loads[2].wait()

    def tab(k):
        j = partners[0, 2 * k + rep]
        use = j >= 0
        j = jnp.where(use, j, own)
        o = [wrap(corners[d, own] - corners[d, j]) for d in range(3)]
        dz = lax.div(j, n_orb) - here_z
        dz = jnp.where(dz > n_slab // 2, dz - n_slab, jnp.where(dz < -(n_slab // 2), dz + n_slab, dz))
        dz = jnp.clip(dz, -HALO, HALO)
        return ((dz + HALO) * n_orb + lax.rem(j, n_orb)) * 16, o[2], o[1], o[0], use

    shift_boxes(pool, tab, zero_plane, blocks * 16, m)
    densities(m, cen, yh, yl)
    for load in loads[3:]:
        load.wait()
    w = [(w_ref[0].at[pl.ds(a, 256)], w_ref[0].at[pl.ds(a + 256, 256)]) for a in (0, 512)]
    w.append((w_ref[1].at[pl.ds(0, 512)], w_ref[1].at[pl.ds(512, 512)]))
    turn(yh, yl, w, s, False)
    energy = filtered(s, yh, yl, ksp, kdp)
    pl.semaphore_wait(ready_two, 2)

    me = 2 * here_x + rep
    ex[me] = jnp.sum(energy, axis=0, keepdims=True)

    def to_slab(step, cross, back):
        other_rep = 1 - rep if cross else rep
        there = 2 * lax.rem(here_x - step + n_orb, n_orb) + other_rep
        cell = ex.at[there if back else me]
        n = 2 * step + cross
        return pltpu.make_async_remote_copy(
            src_ref=cell, dst_ref=cell, send_sem=tail_sem.at[2 + n], recv_sem=tail_sem.at[2 + 2 * n_orb + n],
            device_id={**at_orb(step), "rep": other_rep}, device_id_type=MESH)

    def to_column(step, back):
        cell = ez.at[lax.rem(here_z - step + n_slab, n_slab) if back else here_z]
        first = 2 + 4 * n_orb
        return pltpu.make_async_remote_copy(
            src_ref=cell, dst_ref=cell, send_sem=tail_sem.at[first + step],
            recv_sem=tail_sem.at[first + n_slab + step], device_id=at_slab(step), device_id_type=MESH)
    near = [(step, cross) for step in range(n_orb) for cross in range(2) if step or cross]
    near.sort(key=lambda v: -min(v[0], n_orb - v[0]))
    far = sorted(range(1, n_slab), key=lambda v: -min(v, n_slab - v))
    for step, cross in near:
        to_slab(step, cross, False).start()
    turn(yh, yl, w, s, True)
    collect(s, m, acc)
    res = summed_tiles(acc)
    for t in range(8):
        part[t] = res[t]
    swap_part = pltpu.make_async_remote_copy(
        src_ref=part, dst_ref=other, send_sem=tail_sem.at[0], recv_sem=tail_sem.at[1],
        device_id=sibling, device_id_type=MESH)
    swap_part.start()
    for step, cross in near:
        to_slab(step, cross, True).wait_recv()
    ez[here_z] = functools.reduce(lambda a, b: a + b, [ex[i] for i in range(2 * n_orb)])
    for step in far:
        to_column(step, False).start()
    swap_part.wait()
    for t in range(8):
        kern[:, LANES * t:LANES * t + LANES] = -swap_tile(part[t] + other[t])
    flush = pltpu.make_async_copy(kern, out_ref.at[0], local_sem.at[0])
    flush.start()
    for step, cross in near:
        to_slab(step, cross, False).wait_send()
    for step in far:
        to_column(step, True).wait_recv()
    total = functools.reduce(lambda a, b: a + b, [ez[i] for i in range(n_slab)])
    for step in far:
        to_column(step, False).wait_send()
    flush.wait()
    en_ref[0] = jnp.sum(total) * np.float32(-1.0 / (2.0 * n_slab * n_orb * B ** 3))


def body(n_slab, n_orb, orbitals, corners, partners, kernel):
    blocks = (2 * HALO + 1) * n_orb
    smem = pl.BlockSpec(memory_space=pltpu.SMEM)
    hbm = pl.BlockSpec(memory_space=pl.ANY)
    dma = pltpu.SemaphoreType.DMA
    tables = plane_tables()
    weights = [jnp.asarray(np.concatenate(tables[:4])), jnp.asarray(np.concatenate(tables[4:]))]
    return pl.pallas_call(
        functools.partial(kernel_body, n_slab, n_orb),
        out_shape=(jax.ShapeDtypeStruct((1, B, B * B), F32), jax.ShapeDtypeStruct((1,), F32)),
        in_specs=[hbm] * 6,
        out_specs=(hbm, smem),
        scratch_shapes=[
            pltpu.VMEM((2 * blocks * 16 + 1, 8, LANES), BF16),
            pltpu.VMEM((8 * MST, LANES), F32),
            pltpu.VMEM((384, 1024), BF16),
            pltpu.VMEM((384, 1024), BF16),
            pltpu.VMEM((8, 384, LANES), F32),
            pltpu.VMEM((512, LANES), F32),
            pltpu.VMEM((128, LANES), F32),
            pltpu.VMEM((1024, LANES), F32),
            pltpu.VMEM((1024, LANES), F32),
            pltpu.VMEM((B, B * B), F32),
            pltpu.VMEM((8, B, LANES), F32),
            pltpu.VMEM((8, B, LANES), F32),
            pltpu.VMEM((2 * n_orb, 1, LANES), F32),
            pltpu.VMEM((n_slab, 1, LANES), F32),
            *[pltpu.VMEM(w.shape, BF16) for w in weights],
            pltpu.VMEM((1, B, B * B), BF16),
            pltpu.SMEM(corners.shape[::-1], jnp.int32),
            pltpu.SMEM(partners.shape, jnp.int32),
            dma((6,)),
            dma((blocks,)),
            dma((blocks,)),
            dma((blocks,)),
            dma((blocks,)),
            dma((2 + 4 * n_orb + 2 * n_slab,)),
            pltpu.SemaphoreType.REGULAR,
            pltpu.SemaphoreType.REGULAR,
        ],
        compiler_params=pltpu.CompilerParams(
            collective_id=0, has_side_effects=True, vmem_limit_bytes=67043328),
    )(orbitals, corners.T, partners, kernel, *weights)


def solution(mesh):
    in_specs = (
        P(("grp", "slab", "orb"), None, None),
        P("grp", None),
        P(("grp", "slab", "orb"), None),
        P(),
    )
    out_specs = (P(("grp", "slab", "orb"), None, None), P("grp"))
    step = functools.partial(body, mesh.shape["slab"], mesh.shape["orb"])
    return jax.shard_map(step, mesh=mesh, in_specs=in_specs, out_specs=out_specs, check_vma=False)
```
